8 devices in a mesh: dp: 2 (over z, y), ep: 4 (over x, core).
Axes of the slice: x: 2, y: 2, z: 1, core: 2. Of those that a mesh axis runs over, the one named last changes fastest.
Arguments:
- x_rows: bfloat16 [2048, 2048], P(('dp', 'ep')), parts along dimension 0
- logits: float32 [2048, 128], P(('dp', 'ep')), parts along dimension 0
- w_in: bfloat16 [128, 2048, 768], P('ep')
- w_out: bfloat16 [128, 768, 2048], P('ep')
Outputs:
- output: bfloat16 [2048, 2048], P(('dp', 'ep')), parts along dimension 0
There are 2 independent parts. The reference program is written for one: setup_inputs(seed, part) draws one part's arguments, and reference() takes and returns one part's arrays. A program takes and returns all parts, laid end to end along the dimension named above; an argument that names none is the same for every part.
All inputs are finite; a program needn't handle non-finite values.
Results may differ from the reference program's by a relative error of at most 0.001.
Values are sent between devices in bfloat16 or wider.
A program may use at most 1 GiB of HBM per device.

```python
import math
import jax
import jax.numpy as jnp
from jax import lax

TOKENS = 1024
D_MODEL = 2048
FF_HIDDEN = 768
EXPERTS = 128
CAPACITY = 16
GROUP_DEV = 4
LOGIT_SHIFT = int(1024 * math.log(EXPERTS))


def draw_logits(route_key):
    sub_keys = jax.random.split(route_key, 5)
    tok_dev = TOKENS // GROUP_DEV
    mean_cnt = 2 * tok_dev // EXPERTS
    quarter = EXPERTS // 4
    exp_order = jax.random.permutation(sub_keys[0], EXPERTS)
    rot_bits = jax.random.randint(sub_keys[1], (GROUP_DEV,), 0, 2)
    tier_vals = jnp.array([2 * mean_cnt, mean_cnt, mean_cnt // 2, mean_cnt // 2], dtype=jnp.int32)
    tier_idx = (jnp.arange(EXPERTS)[None, :] // quarter + rot_bits[:, None]) % 4
    slot_ends = jnp.cumsum(tier_vals[tier_idx], axis=1)
    slot_ids = jnp.arange(2 * tok_dev)
    rank_pos = jnp.sum((slot_ends[:, None, :] <= slot_ids[None, :, None]).astype(jnp.int32), axis=2)
    pick_list = exp_order[rank_pos]
    perm_keys = jax.random.split(sub_keys[2], GROUP_DEV)
    tok_perm = jax.vmap(lambda perm_key: jax.random.permutation(perm_key, tok_dev))(perm_keys)
    first_pick = jnp.take_along_axis(pick_list[:, :tok_dev], tok_perm, axis=1).reshape(TOKENS)
    second_pick = jnp.take_along_axis(pick_list[:, tok_dev:], tok_perm, axis=1).reshape(TOKENS)
    expert_ids = jnp.arange(EXPERTS)
    chosen = (expert_ids[None, :] == first_pick[:, None]) | (expert_ids[None, :] == second_pick[:, None])
    base_val = jax.random.randint(sub_keys[3], (TOKENS, EXPERTS), 0, 2048)
    pick_val = jax.random.randint(sub_keys[4], (TOKENS, EXPERTS), 1024, 3072) + LOGIT_SHIFT
    score_int = jnp.where(chosen, pick_val, base_val) * EXPERTS + expert_ids[None, :]
    return score_int.astype(jnp.float32) / (1024.0 * EXPERTS)


def setup_inputs(seed: int = 0, part: int = 0) -> dict:
    part_key = jax.random.fold_in(jax.random.key(seed), part)
    sub_keys = jax.random.split(part_key, 2)
    w_keys = jax.random.split(jax.random.key(seed + 1), 2)
    x_rows = jax.random.normal(sub_keys[0], (TOKENS, D_MODEL), jnp.float32).astype(jnp.bfloat16)
    logits = draw_logits(sub_keys[1])
    w_in = (jax.random.normal(w_keys[0], (EXPERTS, D_MODEL, FF_HIDDEN), jnp.float32) * D_MODEL ** -0.5).astype(jnp.bfloat16)
    w_out = (jax.random.normal(w_keys[1], (EXPERTS, FF_HIDDEN, D_MODEL), jnp.float32) * (2.0 * FF_HIDDEN ** -0.5)).astype(jnp.bfloat16)
    return {'x_rows': x_rows, 'logits': logits, 'w_in': w_in, 'w_out': w_out}


def reference(x_rows, logits, w_in, w_out):
    gate_probs = jax.nn.softmax(logits, axis=-1)
    top_vals, top_ids = lax.top_k(logits, 2)
    chosen = (logits >= top_vals[:, 1:2]).astype(jnp.int32)
    before = jnp.cumsum(chosen, axis=0) - chosen
    pick_pos = jnp.take_along_axis(before, top_ids, axis=1)
    dest_row = jnp.where(pick_pos < CAPACITY, top_ids * CAPACITY + pick_pos, EXPERTS * CAPACITY)
    tok_ids = jnp.broadcast_to(jnp.arange(TOKENS, dtype=jnp.int32)[:, None], (TOKENS, 2))
    slot_tok = jnp.full((EXPERTS * CAPACITY,), TOKENS, jnp.int32).at[dest_row.reshape(-1)].set(tok_ids.reshape(-1), mode='drop')
    expert_rows = jnp.take(x_rows, slot_tok, axis=0, mode='fill', fill_value=0).reshape(EXPERTS, CAPACITY, D_MODEL)

    def expert_ffn(operands):
        rows_in, w_first, w_second = operands
        hidden = jax.nn.gelu(jnp.dot(rows_in, w_first, preferred_element_type=jnp.float32), approximate=True).astype(jnp.bfloat16)
        return jnp.dot(hidden, w_second, preferred_element_type=jnp.float32).astype(jnp.bfloat16)

    expert_out = lax.map(expert_ffn, (expert_rows, w_in, w_out)).reshape(EXPERTS * CAPACITY, D_MODEL)
    rows_back = jnp.take(expert_out, dest_row, axis=0, mode='fill', fill_value=0)
    pick_gate = jnp.take_along_axis(gate_probs, top_ids, axis=1)
    mix_sum = jnp.sum(pick_gate[:, :, None] * rows_back.astype(jnp.float32), axis=1)
    return (x_rows.astype(jnp.float32) + mix_sum).astype(jnp.bfloat16)
```

```python
import functools

import jax
import jax.numpy as jnp
from jax import lax
from jax.experimental import pallas as pl
from jax.experimental.pallas import tpu as pltpu
from jax.sharding import PartitionSpec as P

MESH = pl.DeviceIdType.MESH
RING = 6
CHUNKS = 4
LAG = 4


def moe_kernel(cfg, x_hbm, logits_ref, w1_hbm, w2_hbm, out_ref,
               x_all, masks, rows_in, z_all, pick_in, pick_out, w1_buf, w2_buf,
               w1_sem, w2_sem, own_sem, x_send, x_recv, m_send, m_recv, z_send, z_recv):
    tok, d_model, d_ff, experts, exp_dev, cap = cfg
    me = lax.axis_index("ep")
    core = me % 2
    partner = me + 1 - 2 * core
    xn = (me + 2) % 4
    diag = 3 - me
    bf16, f32 = jnp.bfloat16, jnp.float32

    def w1_copy(e):
        return pltpu.make_async_copy(w1_hbm.at[e], w1_buf.at[e % RING], w1_sem.at[e % RING])

    def w2_copy(e):
        return pltpu.make_async_copy(w2_hbm.at[e], w2_buf.at[e % RING], w2_sem.at[e % RING])

    def remote(src, dst, send, recv, dev):
        return pltpu.make_async_remote_copy(src_ref=src, dst_ref=dst, send_sem=send, recv_sem=recv,
                                            device_id={"ep": dev}, device_id_type=MESH)

    w1_copy(0).start()
    w2_copy(0).start()

    barrier = pltpu.get_barrier_semaphore()
    for peer in (partner, xn, diag):
        pl.semaphore_signal(barrier, inc=1, device_id={"ep": peer}, device_id_type=MESH)
    pl.semaphore_wait(barrier, 3)

    piece = tok // CHUNKS
    near = pl.multiple_of(core * tok, tok)
    far = pl.multiple_of(2 * tok + core * tok, tok)

    def x_far(k):
        return remote(x_hbm.at[pl.ds(k * piece, piece)], x_all.at[pl.ds(far + k * piece, piece)],
                      x_send.at[0, k], x_recv.at[0, k], xn)

    def x_fwd(k):
        here = x_all.at[pl.ds(far + k * piece, piece)]
        return remote(here, here, x_send.at[1, k], x_recv.at[1, k], partner)

    x_near = remote(x_hbm, x_all.at[pl.ds(near, tok)], x_send.at[2, 0], x_recv.at[2, 0], partner)
    own = pltpu.make_async_copy(x_hbm, x_all.at[pl.ds(near, tok)], own_sem)
    x_far(0).start()
    own.start()
    x_near.start()
    for e in range(1, RING):
        w1_copy(e).start()
        w2_copy(e).start()

    logits = logits_ref[...]
    lane = lax.broadcasted_iota(jnp.int32, (tok, experts), 1).astype(f32)
    top1 = jnp.max(logits, axis=1, keepdims=True)
    is1 = logits == top1
    rest = jnp.where(is1, -jnp.inf, logits)
    top2 = jnp.max(rest, axis=1, keepdims=True)
    is2 = rest == top2
    chosen = jnp.where(is1 | is2, 1.0, 0.0)
    masks[me] = chosen.T.astype(bf16)
    total = jnp.sum(jnp.exp(logits - top1), axis=1, keepdims=True)
    gate1 = 1.0 / total
    gate2 = jnp.exp(top2 - top1) / total
    row_id = lax.broadcasted_iota(jnp.int32, (tok, tok), 0)
    col_id = lax.broadcasted_iota(jnp.int32, (tok, tok), 1)
    lower = jnp.where(col_id < row_id, 1.0, 0.0).astype(bf16)
    upper = jnp.where(row_id < col_id, 1.0, 0.0).astype(bf16)
    before = jnp.dot(lower, chosen.astype(bf16), preferred_element_type=f32)

    peers = (partner, xn, diag)

    def mask_copy(i):
        return remote(masks.at[me], masks.at[me], m_send.at[i], m_recv.at[i], peers[i])

    for i in range(3):
        mask_copy(i).start()
    for k in range(1, CHUNKS):
        x_far(k).start()
    for i in range(3):
        remote(masks.at[peers[i]], masks.at[peers[i]], m_send.at[i], m_recv.at[i], peers[i]).wait_recv()

    ones = jnp.ones((8, tok), bf16)
    offset = jnp.zeros((8, experts), f32)
    for d in range(4):
        count = lax.dot_general(ones, masks[d], (((1,), (1,)), ((), ())), preferred_element_type=f32)
        offset = offset + jnp.where(d < me, 1.0, 0.0) * count
    position = before + offset[0:1, :]
    slot_lane = lax.broadcasted_iota(jnp.int32, (tok, experts * cap), 1).astype(f32)
    for i, hot in enumerate((is1, is2)):
        pos = jnp.sum(jnp.where(hot, position, 0.0), axis=1, keepdims=True)
        exp_id = jnp.sum(jnp.where(hot, lane, 0.0), axis=1, keepdims=True)
        slot = jnp.where(pos < cap, exp_id * cap + pos, -1.0)
        pick_out[i * tok:(i + 1) * tok, :] = jnp.where(slot_lane == slot, 1.0, 0.0).astype(bf16)

    first = pl.multiple_of(me * exp_dev, exp_dev)
    running = jnp.zeros((exp_dev, 1), f32)
    slot_id = lax.broadcasted_iota(jnp.int32, (exp_dev, cap, tok), 1).astype(f32)
    for d in range(4):
        m = masks[d, pl.ds(first, exp_dev), :]
        m32 = m.astype(f32)
        pos = jnp.dot(m, upper, preferred_element_type=f32) + running
        pos = jnp.where(m32 > 0.5, pos, -1.0)
        running = running + jnp.sum(m32, axis=1, keepdims=True)
        hot = jnp.where(pos[:, None, :] == slot_id, 1.0, 0.0).reshape(exp_dev * cap, tok).astype(bf16)
        side = (d // 2 + me // 2) % 2
        pick_in[side, :, (d % 2) * tok:(d % 2 + 1) * tok] = hot

    own.wait()
    x_near.wait_recv()
    width = 256

    def gather_near(j, c):
        cols = pl.ds(pl.multiple_of(j * width, width), width)
        rows_in[:, cols] = jnp.dot(pick_in[0], x_all[0:2 * tok, cols], preferred_element_type=f32).astype(bf16)
        return c

    lax.fori_loop(0, d_model // width, gather_near, 0)

    for k in range(CHUNKS):
        x_far(k).wait_recv()
        x_fwd(k).start()
    for k in range(CHUNKS):
        x_fwd(k).wait_recv()

    def gather_far(j, c):
        cols = pl.ds(pl.multiple_of(j * width, width), width)
        rows = jnp.dot(pick_in[1], x_all[2 * tok:4 * tok, cols], preferred_element_type=f32)
        rows_in[:, cols] = (rows_in[:, cols].astype(f32) + rows).astype(bf16)
        return c

    lax.fori_loop(0, d_model // width, gather_far, 0)

    def z_rows(dev, e):
        return z_all.at[pl.ds(pl.multiple_of((dev * exp_dev + e) * cap, cap), cap)]

    def z_copy(i, e):
        dev, src = ((partner, me), (xn, me), (partner, xn))[i]
        return remote(z_rows(src, e), z_rows(src, e), z_send.at[i, e], z_recv.at[i, e], dev)

    def forward(e):
        z_copy(1, e).wait_recv()
        z_copy(2, e).start()

    def expert(e, c):
        slot = e % RING
        w1_copy(e).wait()
        rows = rows_in[pl.ds(pl.multiple_of(e * cap, cap), cap), :]
        hidden = jnp.dot(rows, w1_buf[slot], preferred_element_type=f32)
        hidden = jax.nn.gelu(hidden, approximate=True).astype(bf16)

        @pl.when(e + RING < exp_dev)
        def _():
            w1_copy(e + RING).start()

        @pl.when(e >= 1)
        def _():
            z_copy(1, e - 1).start()
            z_copy(0, e - 1).start()

        @pl.when(e >= LAG)
        def _():
            forward(e - LAG)

        w2_copy(e).wait()
        z = jnp.dot(hidden, w2_buf[slot], preferred_element_type=f32).astype(bf16)
        z_all[pl.ds(pl.multiple_of((me * exp_dev + e) * cap, cap), cap), :] = z

        @pl.when(e + RING < exp_dev)
        def _():
            w2_copy(e + RING).start()
        return c

    lax.fori_loop(0, exp_dev, expert, 0)
    z_copy(1, exp_dev - 1).start()
    z_copy(0, exp_dev - 1).start()
    for e in range(exp_dev - LAG, exp_dev):
        forward(e)

    def drain(e, c):
        z_copy(0, e).wait_recv()
        z_copy(2, e).wait_recv()
        for i in range(3):
            z_copy(i, e).wait_send()
        return c

    lax.fori_loop(0, exp_dev, drain, 0)

    def combine(j, c):
        cols = pl.ds(pl.multiple_of(j * width, width), width)
        back = jnp.dot(pick_out[...], z_all[:, cols], preferred_element_type=f32)
        mix = gate1 * back[:tok] + gate2 * back[tok:]
        mine = x_all[pl.ds(near, tok), cols].astype(f32)
        out_ref[:, cols] = (mine + mix).astype(bf16)
        return c

    lax.fori_loop(0, d_model // width, combine, 0)
    x_near.wait_send()
    for k in range(CHUNKS):
        x_far(k).wait_send()
        x_fwd(k).wait_send()
    for i in range(3):
        mask_copy(i).wait_send()


def solution(mesh):
    group = mesh.shape["ep"]
    row_spec = P(("dp", "ep"), None)
    expert_spec = P("ep", None, None)

    def local_step(x_rows, logits, w_in, w_out):
        tok, d_model = x_rows.shape
        experts = logits.shape[1]
        exp_dev, _, d_ff = w_in.shape
        cap = 2 * tok * group // experts
        cfg = (tok, d_model, d_ff, experts, exp_dev, cap)
        bf16 = jnp.bfloat16
        hbm = pl.BlockSpec(memory_space=pl.ANY)
        vmem = pl.BlockSpec(memory_space=pltpu.VMEM)
        dma = pltpu.SemaphoreType.DMA
        return pl.pallas_call(
            functools.partial(moe_kernel, cfg),
            name="moe",
            out_shape=jax.ShapeDtypeStruct((tok, d_model), bf16),
            in_specs=[hbm, vmem, hbm, hbm],
            out_specs=vmem,
            scratch_shapes=[
                pltpu.VMEM((group * tok, d_model), bf16),
                pltpu.VMEM((group, experts, tok), bf16),
                pltpu.VMEM((exp_dev * cap, d_model), bf16),
                pltpu.VMEM((experts * cap, d_model), bf16),
                pltpu.VMEM((2, exp_dev * cap, 2 * tok), bf16),
                pltpu.VMEM((2 * tok, experts * cap), bf16),
                pltpu.VMEM((RING, d_model, d_ff), bf16),
                pltpu.VMEM((RING, d_ff, d_model), bf16),
                dma((RING,)), dma((RING,)), dma,
                dma((3, CHUNKS)), dma((3, CHUNKS)),
                dma((3,)), dma((3,)),
                dma((3, exp_dev)), dma((3, exp_dev)),
            ],
            compiler_params=pltpu.CompilerParams(
                collective_id=0, has_side_effects=True, vmem_limit_bytes=66_000_000),
        )(x_rows, logits, w_in, w_out)

    return jax.shard_map(local_step, mesh=mesh, in_specs=(row_spec, row_spec, expert_spec, expert_spec),
                         out_specs=row_spec, check_vma=False)
```

```python
import functools

import jax
import jax.numpy as jnp
from jax import lax
from jax.experimental import pallas as pl
from jax.experimental.pallas import tpu as pltpu
from jax.sharding import PartitionSpec as P

MESH = pl.DeviceIdType.MESH
PARTS = 4
W2_RING = 5
UNROLL = 4
X_CHUNKS = 8
PIECE = 4


def moe_kernel(cfg, x_hbm, logits_hbm, w1_hbm, w2_hbm, out_ref,
               logits_ref, x_all, masks, rows_in, hid, z_all, mix, gates, pick_in, pick_out, w1_buf, w2_buf,
               w1_sem, w2_sem, own_sem, x_send, x_recv, m_send, m_recv, z_send, z_recv):
    tok, d_model, d_ff, experts, exp_dev, cap = cfg
    me = lax.axis_index("ep")
    core = me % 2
    partner = me + 1 - 2 * core
    xn = (me + 2) % 4
    bf16, f32 = jnp.bfloat16, jnp.float32
    part = d_model // PARTS

    def remote(src, dst, send, recv, dev):
        return pltpu.make_async_remote_copy(src_ref=src, dst_ref=dst, send_sem=send, recv_sem=recv,
                                            device_id={"ep": dev}, device_id_type=MESH)

    barrier = pltpu.get_barrier_semaphore()
    for peer in (xn, partner):
        pl.semaphore_signal(barrier, inc=1, device_id={"ep": peer}, device_id_type=MESH)
    get_logits = pltpu.make_async_copy(logits_hbm, logits_ref, own_sem.at[1])
    get_logits.start()

    def w1_copy(c, e):
        rows = pl.ds(pl.multiple_of(c * part, part), part)
        return pltpu.make_async_copy(w1_hbm.at[e, rows], w1_buf.at[e], w1_sem.at[e])

    def w2_copy(e):
        return pltpu.make_async_copy(w2_hbm.at[e], w2_buf.at[e % W2_RING], w2_sem.at[e % W2_RING])

    def w1_start(e, carry):
        w1_copy(0, e).start()
        return carry

    lax.fori_loop(0, 4, w1_start, 0)

    get_logits.wait()
    logits = logits_ref[...]
    top1 = jnp.max(logits, axis=1, keepdims=True)
    is1 = logits == top1
    rest = jnp.where(is1, -jnp.inf, logits)
    top2 = jnp.max(rest, axis=1, keepdims=True)
    is2 = rest == top2
    chosen = jnp.where(is1 | is2, 1.0, 0.0)
    masks[me] = chosen.T.astype(bf16)
    row_id = lax.broadcasted_iota(jnp.int32, (tok, tok), 0)
    col_id = lax.broadcasted_iota(jnp.int32, (tok, tok), 1)
    lower = jnp.where(col_id < row_id, 1.0, 0.0).astype(bf16)
    upper = jnp.where(row_id < col_id, 1.0, 0.0).astype(bf16)
    before = jnp.dot(lower, chosen.astype(bf16), preferred_element_type=f32)

    def mask_copy(i):
        dev, src = ((partner, me), (xn, me), (partner, xn))[i]
        return remote(masks.at[src], masks.at[src], m_send.at[i], m_recv.at[i], dev)

    width = d_model // X_CHUNKS
    near = pl.multiple_of(core * tok, tok)
    far = pl.multiple_of(2 * tok + core * tok, tok)

    def x_far(k):
        cols = pl.ds(k * width, width)
        return remote(x_hbm.at[:, cols], x_all.at[pl.ds(far, tok), cols], x_send.at[0, k], x_recv.at[0, k], xn)

    def x_fwd(k):
        here = x_all.at[pl.ds(far, tok), pl.ds(k * width, width)]
        return remote(here, here, x_send.at[1, k], x_recv.at[1, k], partner)

    x_near = remote(x_hbm, x_all.at[pl.ds(near, tok)], x_send.at[2, 0], x_recv.at[2, 0], partner)
    own = pltpu.make_async_copy(x_hbm, x_all.at[pl.ds(near, tok)], own_sem.at[0])
    pl.semaphore_wait(barrier, 2)
    mask_copy(1).start()
    for k in range(X_CHUNKS):
        x_far(k).start()
    mask_copy(0).start()
    own.start()
    x_near.start()
    lax.fori_loop(4, exp_dev, w1_start, 0)
    for e in range(W2_RING):
        w2_copy(e).start()

    total = jnp.sum(jnp.exp(logits - top1), axis=1, keepdims=True)
    gates[0] = jnp.broadcast_to(1.0 / total, (tok, 128))
    gates[1] = jnp.broadcast_to(jnp.exp(top2 - top1) / total, (tok, 128))
    mix[...] = jnp.zeros_like(mix)
    mask_copy(1).wait_recv()
    mask_copy(2).start()
    mask_copy(0).wait_recv()
    mask_copy(2).wait_recv()

    first = pl.multiple_of(me * exp_dev, exp_dev)
    running = jnp.zeros((exp_dev, 1), f32)
    slot_id = lax.broadcasted_iota(jnp.int32, (exp_dev, cap, tok), 1).astype(f32)
    for d in range(4):
        m = masks[d, pl.ds(first, exp_dev), :]
        m32 = m.astype(f32)
        pos = jnp.dot(m, upper, preferred_element_type=f32) + running
        pos = jnp.where(m32 > 0.5, pos, -1.0)
        running = running + jnp.sum(m32, axis=1, keepdims=True)
        hot = jnp.where(pos[:, None, :] == slot_id, 1.0, 0.0).reshape(exp_dev * cap, tok).astype(bf16)
        side = (d // 2 + me // 2) % 2
        pick_in[side, :, (d % 2) * tok:(d % 2 + 1) * tok] = hot

    ones = jnp.ones((8, tok), bf16)
    offset = jnp.zeros((8, experts), f32)
    for d in range(4):
        count = lax.dot_general(ones, masks[d], (((1,), (1,)), ((), ())), preferred_element_type=f32)
        offset = offset + jnp.where(d < me, 1.0, 0.0) * count
    position = before + offset[0:1, :]
    lane = lax.broadcasted_iota(jnp.int32, (tok, experts), 1)
    dev_id, exp_id = lane // exp_dev, lane % exp_dev
    base = (((exp_id // PIECE) * 4 + dev_id) * PIECE + exp_id % PIECE) * cap
    base = base.astype(f32)
    slot_lane = lax.broadcasted_iota(jnp.int32, (tok, experts * cap), 1).astype(f32)
    for i, hot in enumerate((is1, is2)):
        pos = jnp.sum(jnp.where(hot, position, 0.0), axis=1, keepdims=True)
        start = jnp.sum(jnp.where(hot, base, 0.0), axis=1, keepdims=True)
        slot = jnp.where(pos < cap, start + pos, -1.0)
        pick_out[i * tok:(i + 1) * tok, :] = jnp.where(slot_lane == slot, 1.0, 0.0).astype(bf16)

    own.wait()
    x_near.wait_recv()

    def pass_on(k):
        x_far(k).wait_recv()
        x_fwd(k).start()

    def gather(k):
        x_fwd(k).wait_recv()
        cols = slice(k * width, (k + 1) * width)
        rows = jnp.dot(pick_in[0], x_all[0:2 * tok, cols], preferred_element_type=f32)
        rows = rows + jnp.dot(pick_in[1], x_all[2 * tok:4 * tok, cols], preferred_element_type=f32)
        rows_in[:, cols] = rows.astype(bf16)

    pass_on(0)
    for c in range(PARTS):
        pass_on(2 * c + 1)
        gather(2 * c)
        gather(2 * c + 1)
        if c == PARTS - 1:
            break

        def first_product(g, carry):
            for i in range(UNROLL):
                w1_copy(c, g * UNROLL + i).wait()
            for i in range(UNROLL):
                e = g * UNROLL + i
                rows = rows_in[pl.ds(pl.multiple_of(e * cap, cap), cap), c * part:(c + 1) * part]
                h = jnp.dot(rows, w1_buf[e], preferred_element_type=f32)
                hid[e] = h if c == 0 else hid[e] + h
            for i in range(UNROLL):
                w1_copy(c + 1, g * UNROLL + i).start()
            return carry

        steps = exp_dev // UNROLL
        lax.fori_loop(0, steps // 2, first_product, 0)
        pass_on(2 * c + 2)
        lax.fori_loop(steps // 2, steps, first_product, 0)

    def z_rows(dev, e):
        start = (((e // PIECE) * 4 + dev) * PIECE + e % PIECE) * cap
        return pl.ds(pl.multiple_of(start, cap), cap)

    def z_copy(i, e):
        dev, src = ((partner, me), (xn, me), (partner, xn))[i]
        rows = z_all.at[z_rows(src, e)]
        return remote(rows, rows, z_send.at[i, e], z_recv.at[i, e], dev)

    def forward(e):
        z_copy(1, e).wait_recv()
        z_copy(2, e).start()

    def send(e):
        z_copy(1, e).start()
        z_copy(0, e).start()

    def combine(p):
        for i in range(PIECE):
            z_copy(0, p * PIECE + i).wait_recv()
            z_copy(2, p * PIECE + i).wait_recv()
        depth = 4 * PIECE * cap
        rows = pl.ds(pl.multiple_of(p * depth, depth), depth)
        block = 512
        gate1 = jnp.concatenate([gates[0]] * (block // 128), axis=1)
        gate2 = jnp.concatenate([gates[1]] * (block // 128), axis=1)
        for j in range(d_model // block):
            cols = slice(j * block, (j + 1) * block)
            back = jnp.dot(pick_out[:, rows], z_all[rows, cols], preferred_element_type=f32)
            mix[:, cols] += gate1 * back[:tok] + gate2 * back[tok:]

    def expert(e, carry):
        @pl.when(e >= 1)
        def _():
            send(e - 1)

        w1_copy(PARTS - 1, e).wait()
        rows = rows_in[pl.ds(pl.multiple_of(e * cap, cap), cap), (PARTS - 1) * part:]
        h = hid[e] + jnp.dot(rows, w1_buf[e], preferred_element_type=f32)
        hidden = jax.nn.gelu(h, approximate=True).astype(bf16)

        @pl.when((e >= 5) & ((2 * e) // 3 != (2 * e - 2) // 3))
        def _():
            forward((2 * e) // 3 - 3)

        w2_copy(e).wait()
        z = jnp.dot(hidden, w2_buf[e % W2_RING], preferred_element_type=f32).astype(bf16)
        z_all[z_rows(me, e), :] = z

        @pl.when(e + W2_RING < exp_dev)
        def _():
            w2_copy(e + W2_RING).start()

        @pl.when((e >= 11) & (e % 6 == 5))
        def _():
            combine(e // 6 - 1)
        return carry

    lax.fori_loop(0, exp_dev, expert, 0)
    send(exp_dev - 1)
    done = (2 * (exp_dev - 1)) // 3 - 2
    pieces = exp_dev // PIECE

    def forward_step(e, carry):
        forward(e)
        return carry

    lax.fori_loop(done, pieces // 2 * PIECE + PIECE, forward_step, 0)

    def last_pieces(p, carry):
        @pl.when(p < pieces - 1)
        def _():
            lax.fori_loop((p + 1) * PIECE, (p + 2) * PIECE, forward_step, 0)
        combine(p)
        return carry

    lax.fori_loop(pieces // 2, pieces, last_pieces, 0)
    out_ref[...] = (x_all[pl.ds(near, tok), :].astype(f32) + mix[...]).astype(bf16)

    def drain(e, carry):
        for i in range(3):
            z_copy(i, e).wait_send()
        return carry

    lax.fori_loop(0, exp_dev, drain, 0)
    x_near.wait_send()
    for k in range(X_CHUNKS):
        x_far(k).wait_send()
        x_fwd(k).wait_send()
    for i in range(3):
        mask_copy(i).wait_send()


def solution(mesh):
    group = mesh.shape["ep"]
    row_spec = P(("dp", "ep"), None)
    expert_spec = P("ep", None, None)

    def local_step(x_rows, logits, w_in, w_out):
        tok, d_model = x_rows.shape
        experts = logits.shape[1]
        exp_dev, _, d_ff = w_in.shape
        cap = 2 * tok * group // experts
        cfg = (tok, d_model, d_ff, experts, exp_dev, cap)
        bf16 = jnp.bfloat16
        hbm = pl.BlockSpec(memory_space=pl.ANY)
        vmem = pl.BlockSpec(memory_space=pltpu.VMEM)
        dma = pltpu.SemaphoreType.DMA
        return pl.pallas_call(
            functools.partial(moe_kernel, cfg),
            name="moe",
            out_shape=jax.ShapeDtypeStruct((tok, d_model), bf16),
            in_specs=[hbm, hbm, hbm, hbm],
            out_specs=vmem,
            scratch_shapes=[
                pltpu.VMEM((tok, experts), jnp.float32),
                pltpu.VMEM((group * tok, d_model), bf16),
                pltpu.VMEM((group, experts, tok), bf16),
                pltpu.VMEM((exp_dev * cap, d_model), bf16),
                pltpu.VMEM((exp_dev, cap, d_ff), jnp.float32),
                pltpu.VMEM((experts * cap, d_model), bf16),
                pltpu.VMEM((tok, d_model), jnp.float32),
                pltpu.VMEM((2, tok, 128), jnp.float32),
                pltpu.VMEM((2, exp_dev * cap, 2 * tok), bf16),
                pltpu.VMEM((2 * tok, experts * cap), bf16),
                pltpu.VMEM((exp_dev, d_model // PARTS, d_ff), bf16),
                pltpu.VMEM((W2_RING, d_ff, d_model), bf16),
                dma((exp_dev,)), dma((W2_RING,)), dma((2,)),
                dma((3, X_CHUNKS)), dma((3, X_CHUNKS)),
                dma((3,)), dma((3,)),
                dma((3, exp_dev)), dma((3, exp_dev)),
            ],
            compiler_params=pltpu.CompilerParams(
                collective_id=0, has_side_effects=True, vmem_limit_bytes=66_000_000),
        )(x_rows, logits, w_in, w_out)

    return jax.shard_map(local_step, mesh=mesh, in_specs=(row_spec, row_spec, expert_spec, expert_spec),
                         out_specs=row_spec, check_vma=False)
```

```python
import functools

import jax
import jax.numpy as jnp
from jax import lax
from jax.experimental import pallas as pl
from jax.experimental.pallas import tpu as pltpu
from jax.sharding import PartitionSpec as P

MESH = pl.DeviceIdType.MESH
PARTS = 4
W2_RING = 5
UNROLL = 2
SLOTS = 8
X_CHUNKS = ((0, 256), (256, 256), (512, 256), (768, 256), (1024, 256), (1280, 256), (1536, 256), (1792, 128), (1920, 128))


def moe_kernel(cfg, x_hbm, logits_hbm, w1_hbm, w2_hbm, out_hbm,
               logits_ref, x_all, mask_t, mask_out, masks, rows_in, hid, z_out, z_in, mix, gates, pick_in, pick_out,
               w1_buf, w2_buf,
               w1_sem, w2_sem, own_sem, x_send, x_recv, m_send, m_recv, z_send, z_recv):
    tok, d_model, d_ff, experts, exp_dev, cap = cfg
    me = lax.axis_index("ep")
    core = me % 2
    partner = me + 1 - 2 * core
    xn = (me + 2) % 4
    diag = 3 - me
    peers = (xn, diag, partner)
    bf16, f32 = jnp.bfloat16, jnp.float32
    part = d_model // PARTS
    pairs = exp_dev // 2
    row16 = 2 * SLOTS

    def remote(src, dst, send, recv, dev):
        return pltpu.make_async_remote_copy(src_ref=src, dst_ref=dst, send_sem=send, recv_sem=recv,
                                            device_id={"ep": dev}, device_id_type=MESH)

    barrier = pltpu.get_barrier_semaphore()
    for peer in peers:
        pl.semaphore_signal(barrier, inc=1, device_id={"ep": peer}, device_id_type=MESH)
    get_logits = pltpu.make_async_copy(logits_hbm, logits_ref, own_sem.at[1])
    get_logits.start()

    def w1_copy(c, q, to=None):
        to = q if to is None else to
        rows = pl.ds(pl.multiple_of(c * part, part), part)
        return pltpu.make_async_copy(w1_hbm.at[pl.ds(2 * q, 2), rows], w1_buf.at[to], w1_sem.at[to])

    def w2_copy(e):
        return pltpu.make_async_copy(w2_hbm.at[e], w2_buf.at[e % W2_RING], w2_sem.at[e % W2_RING])

    def w1_start(q, carry):
        w1_copy(0, q).start()
        return carry

    lax.fori_loop(0, 2, w1_start, 0)

    def x_block(dev):
        return pl.ds(pl.multiple_of(dev * tok, tok), tok)

    def x_far(k):
        cols = pl.ds(*X_CHUNKS[k])
        return remote(x_hbm.at[:, cols], x_all.at[x_block(me), cols], x_send.at[0], x_recv.at[0, k], xn)

    def x_fwd(k):
        here = x_all.at[x_block(xn), pl.ds(*X_CHUNKS[k])]
        return remote(here, here, x_send.at[1], x_recv.at[1, k], partner)

    x_near = remote(x_hbm, x_all.at[x_block(me)], x_send.at[2], own_sem.at[2], partner)
    own = pltpu.make_async_copy(x_hbm, x_all.at[x_block(me)], own_sem.at[0])
    pl.semaphore_wait(barrier, 3)
    x_far(0).start()
    x_near.start()
    own.start()

    get_logits.wait()
    logits = logits_ref[...]
    top1 = jnp.max(logits, axis=1, keepdims=True)
    is1 = logits == top1
    rest = jnp.where(is1, -jnp.inf, logits)
    top2 = jnp.max(rest, axis=1, keepdims=True)
    is2 = rest == top2
    chosen = jnp.where(is1 | is2, 1.0, 0.0)
    mask_t[...] = chosen.T.astype(bf16)
    counts = jnp.sum(chosen, axis=0, keepdims=True)
    counts = jnp.broadcast_to(jnp.concatenate([counts] * (tok // experts), axis=1), (16, tok)).astype(bf16)
    for i, dev in enumerate(peers + (me,)):
        mask_out[i, :exp_dev] = mask_t[pl.ds(pl.multiple_of(dev * exp_dev, exp_dev), exp_dev), :]
        mask_out[i, exp_dev:] = counts
    masks[me] = mask_out[3]

    def mask_copy(i):
        return remote(mask_out.at[i], masks.at[me], m_send.at[i], m_recv.at[i], peers[i])

    for i in range(3):
        mask_copy(i).start()
    for k in range(1, len(X_CHUNKS)):
        x_far(k).start()
    lax.fori_loop(2, pairs, w1_start, 0)
    for e in range(W2_RING):
        w2_copy(e).start()

    row_id = lax.broadcasted_iota(jnp.int32, (tok, tok), 0)
    col_id = lax.broadcasted_iota(jnp.int32, (tok, tok), 1)
    lower = jnp.where(col_id < row_id, 1.0, 0.0).astype(bf16)
    upper = jnp.where(row_id < col_id, 1.0, 0.0).astype(bf16)
    before = jnp.dot(lower, chosen.astype(bf16), preferred_element_type=f32)
    total = jnp.sum(jnp.exp(logits - top1), axis=1, keepdims=True)
    gates[0] = jnp.broadcast_to(1.0 / total, (tok, 128))
    gates[1] = jnp.broadcast_to(jnp.exp(top2 - top1) / total, (tok, 128))
    mix[...] = jnp.zeros_like(mix)

    slot_id = lax.broadcasted_iota(jnp.int32, (exp_dev, SLOTS, tok), 1).astype(f32)

    def picks(dev):
        m = masks[dev, :exp_dev, :]
        pos = jnp.dot(m, upper, preferred_element_type=f32)
        pos = jnp.where(m.astype(f32) > 0.5, pos, -1.0)
        hot = jnp.where(pos[:, None, :] == slot_id, 1.0, 0.0).reshape(exp_dev * SLOTS, tok).astype(bf16)
        pick_in[dev] = hot

    def gather(dev, first, width):
        cols = slice(first, first + width)
        rows = jnp.dot(pick_in[dev], x_all[x_block(dev), cols], preferred_element_type=f32).astype(bf16)
        rows_in[:, pl.ds(pl.multiple_of(dev * row16, row16), row16), cols] = rows.reshape(pairs, row16, width)

    picks(me)
    own.wait()
    for j in range(0, d_model, 512):
        gather(me, j, 512)
    remote(mask_out.at[2], masks.at[partner], m_send.at[2], m_recv.at[2], partner).wait_recv()
    picks(partner)
    x_near.wait_recv()
    for j in range(0, d_model, 512):
        gather(partner, j, 512)
    for i in range(2):
        remote(mask_out.at[i], masks.at[peers[i]], m_send.at[i], m_recv.at[i], peers[i]).wait_recv()
        picks(peers[i])

    def pass_on(k):
        x_far(k).wait_recv()
        x_fwd(k).start()

    def gather_far(k):
        gather(xn, *X_CHUNKS[k])
        x_fwd(k).wait_recv()
        gather(diag, *X_CHUNKS[k])

    pass_on(0)

    offset = jnp.zeros((1, experts), f32)
    for d in range(4):
        offset = offset + jnp.where(d < me, 1.0, 0.0) * masks[d, exp_dev:, :experts].astype(f32)[0:1]
    position = before + offset
    lane = lax.broadcasted_iota(jnp.int32, (tok, experts), 1)
    dev_id, exp_id = lane // exp_dev, lane % exp_dev
    base = (((exp_id // 4) * 4 + dev_id) * 4 + exp_id % 4) * SLOTS
    base = base.astype(f32) + before
    slot_lane = lax.broadcasted_iota(jnp.int32, (tok, experts * SLOTS), 1).astype(f32)
    for i, hot in enumerate((is1, is2)):
        pos = jnp.sum(jnp.where(hot, position, 0.0), axis=1, keepdims=True)
        slot = jnp.sum(jnp.where(hot, base, 0.0), axis=1, keepdims=True)
        slot = jnp.where(pos < cap, slot, -1.0)
        pick_out[i * tok:(i + 1) * tok, :] = jnp.where(slot_lane == slot, 1.0, 0.0).astype(bf16)

    def weave(a, b):
        blocks = []
        for d in range(4):
            blocks += [a[d * row16:d * row16 + SLOTS], b[d * row16 + SLOTS:(d + 1) * row16]]
        return jnp.concatenate(blocks, axis=0)

    def first_part(c, q, at=None):
        at = q if at is None else at
        rows = rows_in[q, :, c * part:(c + 1) * part]
        a = jnp.dot(rows, w1_buf[at, 0], preferred_element_type=f32)
        b = jnp.dot(rows, w1_buf[at, 1], preferred_element_type=f32)
        return weave(a, b)

    early = pairs // 2
    for c in range(PARTS):
        pass_on(2 * c + 1)
        gather_far(2 * c)
        if c == PARTS - 1:
            pass_on(2 * c + 2)
            gather_far(2 * c + 1)
            gather_far(2 * c + 2)
            break
        gather_far(2 * c + 1)

        def first_product(g, carry):
            for i in range(UNROLL):
                w1_copy(c, g * UNROLL + i).wait()
            for i in range(UNROLL):
                q = g * UNROLL + i
                h = first_part(c, q)
                hid[q] = h if c == 0 else hid[q] + h
            for i in range(UNROLL):
                w1_copy(c + 1, g * UNROLL + i).start()
            return carry

        steps = (pairs if c < PARTS - 2 else early) // UNROLL
        lax.fori_loop(0, steps // 2, first_product, 0)
        pass_on(2 * c + 2)
        lax.fori_loop(steps // 2, steps, first_product, 0)

    half = d_model // 2
    units = pairs // 2
    whole = pl.ds(0, d_model)

    def z_rows(dev, q):
        return pl.ds(pl.multiple_of((((q // 2) * 4 + dev) * 2 + q % 2) * row16, row16), row16)

    def z_copy(i, q, c):
        cols = pl.ds(c * half, half)
        src = z_out.at[q, pl.ds(pl.multiple_of(peers[i] * row16, row16), row16), cols]
        return remote(src, z_in.at[z_rows(me, q), cols], z_send.at[i], z_recv.at[i, z_id(q // 2, c)], peers[i])

    def z_id(u, c):
        return u + jnp.where(u == units - 1, c, 0)

    def unit_wait(u, cols, c):
        for i in range(3):
            rows = pl.ds(pl.multiple_of((u * 4 + peers[i]) * 2 * row16, 2 * row16), 2 * row16)
            here = z_in.at[rows, cols]
            remote(here, here, z_send.at[i], z_recv.at[i, z_id(u, c)], peers[i]).wait_recv()

    def send(q, c):
        for i in range(3):
            z_copy(i, q, c).start()

    def combine(first, depth, lo, hi):
        rows = pl.ds(pl.multiple_of(first, 128), depth)
        block = 512
        gate1 = jnp.concatenate([gates[0]] * (block // 128), axis=1)
        gate2 = jnp.concatenate([gates[1]] * (block // 128), axis=1)
        for j in range(lo, hi, block):
            cols = slice(j, j + block)
            back = jnp.dot(pick_out[:, rows], z_in[rows, cols], preferred_element_type=f32)
            mix[:, cols] += gate1 * back[:tok] + gate2 * back[tok:]

    unit = 4 * 2 * row16

    def finish(q, h):
        hidden = jax.nn.gelu(h, approximate=True).astype(bf16)
        for i in range(2):
            w2_copy(2 * q + i).wait()
        mine = pl.ds(pl.multiple_of(me * row16, row16), row16)
        for c in range(2):
            cols = slice(c * half, (c + 1) * half)
            a = jnp.dot(hidden, w2_buf[(2 * q) % W2_RING, :, cols], preferred_element_type=f32)
            b = jnp.dot(hidden, w2_buf[(2 * q + 1) % W2_RING, :, cols], preferred_element_type=f32)
            z_out[q, :, cols] = weave(a, b).astype(bf16)
            z_in[z_rows(me, q), cols] = z_out[q, mine, cols]
            send(q, c)
        for i in range(2):
            @pl.when(2 * q + i + W2_RING < exp_dev)
            def _():
                w2_copy(2 * q + i + W2_RING).start()

    def units_in(first, count):
        for i in range(count):
            unit_wait(first + i, whole, 0)
        combine(first * unit, count * unit, 0, d_model)

    def early_pair(q, carry):
        w1_copy(PARTS - 1, q).wait()
        h = hid[q] + first_part(PARTS - 1, q)
        w1_copy(PARTS - 1, q + early, q).start()
        finish(q, h)
        return carry

    def late_pair(q, carry):
        w1_copy(PARTS - 2, q).wait()
        h = hid[q] + first_part(PARTS - 2, q)
        w1_copy(PARTS - 1, q, q - early).wait()
        finish(q, h + first_part(PARTS - 1, q, q - early))

        @pl.when((q == 8) | (q == 13))
        def _():
            units_in((q - 8) // 5 * 2, 2)
        return carry

    lax.fori_loop(0, early, early_pair, 0)
    lax.fori_loop(early, pairs, late_pair, 0)

    def later(u, carry):
        units_in(u, 1)
        return carry

    lax.fori_loop(units // 2, units - 1, later, 0)
    block = x_all.at[x_block(me)]
    for i in range(2):
        remote(block, block, x_send.at[i], own_sem.at[2], xn).wait_send()
    x_near.wait_send()
    for i in range(3):
        mask_copy(i).wait_send()

    def out_copy(c):
        cols = pl.ds(c * half, half)
        return pltpu.make_async_copy(x_all.at[x_block(me), cols], out_hbm.at[:, cols], own_sem.at[c])

    for c in range(2):
        cols = slice(c * half, (c + 1) * half)
        unit_wait(units - 1, pl.ds(c * half, half), c)
        combine((units - 1) * unit, unit, c * half, (c + 1) * half)
        x_all[x_block(me), cols] = (x_all[x_block(me), cols].astype(f32) + mix[:, cols]).astype(bf16)
        out_copy(c).start()
    for i in range(3):
        remote(block, block, z_send.at[i], own_sem.at[2], peers[i]).wait_send()
    out_copy(0).wait()
    out_copy(1).wait()


def solution(mesh):
    group = mesh.shape["ep"]
    row_spec = P(("dp", "ep"), None)
    expert_spec = P("ep", None, None)

    def local_step(x_rows, logits, w_in, w_out):
        tok, d_model = x_rows.shape
        experts = logits.shape[1]
        exp_dev, _, d_ff = w_in.shape
        cap = 2 * tok * group // experts
        cfg = (tok, d_model, d_ff, experts, exp_dev, cap)
        bf16 = jnp.bfloat16
        hbm = pl.BlockSpec(memory_space=pl.ANY)
        f32 = jnp.float32
        dma = pltpu.SemaphoreType.DMA
        return pl.pallas_call(
            functools.partial(moe_kernel, cfg),
            name="moe",
            out_shape=jax.ShapeDtypeStruct((tok, d_model), bf16),
            in_specs=[hbm, hbm, hbm, hbm],
            out_specs=hbm,
            scratch_shapes=[
                pltpu.VMEM((tok, experts), f32),
                pltpu.VMEM((group * tok, d_model), bf16),
                pltpu.VMEM((experts, tok), bf16),
                pltpu.VMEM((group, exp_dev + 16, tok), bf16),
                pltpu.VMEM((group, exp_dev + 16, tok), bf16),
                pltpu.VMEM((exp_dev // 2, group * 2 * SLOTS, d_model), bf16),
                pltpu.VMEM((exp_dev // 2, group * 2 * SLOTS, d_ff), f32),
                pltpu.VMEM((exp_dev // 2, group * 2 * SLOTS, d_model), bf16),
                pltpu.VMEM((experts * SLOTS, d_model), bf16),
                pltpu.VMEM((tok, d_model), f32),
                pltpu.VMEM((2, tok, 128), f32),
                pltpu.VMEM((group, exp_dev * SLOTS, tok), bf16),
                pltpu.VMEM((2 * tok, experts * SLOTS), bf16),
                pltpu.VMEM((exp_dev // 2, 2, d_model // PARTS, d_ff), bf16),
                pltpu.VMEM((W2_RING, d_ff, d_model), bf16),
                dma((exp_dev // 2,)), dma((W2_RING,)), dma((3,)),
                dma((3,)), dma((2, len(X_CHUNKS))),
                dma((3,)), dma((3,)),
                dma((3,)), dma((3, exp_dev // 4 + 1)),
            ],
            compiler_params=pltpu.CompilerParams(
                collective_id=0, has_side_effects=True, vmem_limit_bytes=67_000_000),
        )(x_rows, logits, w_in, w_out)

    return jax.shard_map(local_step, mesh=mesh, in_specs=(row_spec, row_spec, expert_spec, expert_spec),
                         out_specs=row_spec, check_vma=False)
```

```python
import functools

import jax
import jax.numpy as jnp
from jax import lax
from jax.experimental import pallas as pl
from jax.experimental.pallas import tpu as pltpu
from jax.sharding import PartitionSpec as P

MESH = pl.DeviceIdType.MESH
PARTS = 4
W2_RING = 5
UNROLL = 2
SLOTS = 8
COPY_CHUNKS = 4
Z_COLS = ((0, 512), (512, 1024), (1536, 512))
X_CHUNKS = ((0, 256), (256, 256), (512, 256), (768, 256), (1024, 256), (1280, 256), (1536, 256), (1792, 128), (1920, 128))


def moe_kernel(cfg, x_hbm, logits_hbm, w1_hbm, w2_hbm, out_hbm,
               logits_ref, x_all, mask_t, mask_out, masks, rows_in, hid, z_out, z_in, mix, gates, pick_in, pick_out,
               w1_buf, w2_buf,
               w1_sem, w2_sem, own_sem, x_send, x_recv, m_send, m_recv, z_send, z_recv):
    tok, d_model, d_ff, experts, exp_dev, cap = cfg
    me = lax.axis_index("ep")
    core = me % 2
    partner = me + 1 - 2 * core
    xn = (me + 2) % 4
    diag = 3 - me
    peers = (xn, diag, partner)
    bf16, f32 = jnp.bfloat16, jnp.float32
    part = d_model // PARTS
    pairs = exp_dev // 2
    row16 = 2 * SLOTS

    def remote(src, dst, send, recv, dev):
        return pltpu.make_async_remote_copy(src_ref=src, dst_ref=dst, send_sem=send, recv_sem=recv,
                                            device_id={"ep": dev}, device_id_type=MESH)

    barrier = pltpu.get_barrier_semaphore()
    for peer in peers:
        pl.semaphore_signal(barrier, inc=1, device_id={"ep": peer}, device_id_type=MESH)
    get_logits = pltpu.make_async_copy(logits_hbm, logits_ref, own_sem.at[1])
    get_logits.start()

    def w1_copy(c, q, to=None):
        to = q if to is None else to
        rows = pl.ds(pl.multiple_of(c * part, part), part)
        return pltpu.make_async_copy(w1_hbm.at[pl.ds(2 * q, 2), rows], w1_buf.at[to], w1_sem.at[to])

    def w2_copy(e):
        return pltpu.make_async_copy(w2_hbm.at[e], w2_buf.at[e % W2_RING], w2_sem.at[e % W2_RING])

    def w1_start(q, carry):
        w1_copy(0, q).start()
        return carry

    lax.fori_loop(0, 2, w1_start, 0)

    def x_block(dev):
        return pl.ds(pl.multiple_of(dev * tok, tok), tok)

    def x_far(k):
        cols = pl.ds(*X_CHUNKS[k])
        return remote(x_hbm.at[:, cols], x_all.at[x_block(me), cols], x_send.at[0], x_recv.at[0, k], xn)

    def x_fwd(k):
        here = x_all.at[x_block(xn), pl.ds(*X_CHUNKS[k])]
        return remote(here, here, x_send.at[1], x_recv.at[1, k], partner)

    x_near = remote(x_hbm, x_all.at[x_block(me)], x_send.at[2], own_sem.at[2], partner)
    own = pltpu.make_async_copy(x_hbm, x_all.at[x_block(me)], own_sem.at[0])
    pl.semaphore_wait(barrier, 3)
    x_far(0).start()
    x_near.start()
    own.start()

    get_logits.wait()
    logits = logits_ref[...]
    top1 = jnp.max(logits, axis=1, keepdims=True)
    is1 = logits == top1
    rest = jnp.where(is1, -jnp.inf, logits)
    top2 = jnp.max(rest, axis=1, keepdims=True)
    is2 = rest == top2
    chosen = jnp.where(is1 | is2, 1.0, 0.0)
    mask_t[...] = chosen.T.astype(bf16)
    counts = jnp.sum(chosen, axis=0, keepdims=True)
    counts = jnp.broadcast_to(jnp.concatenate([counts] * (tok // experts), axis=1), (8, tok)).astype(bf16)
    for i, dev in enumerate(peers + (me,)):
        mask_out[i, :exp_dev] = mask_t[pl.ds(pl.multiple_of(dev * exp_dev, exp_dev), exp_dev), :]
        mask_out[i, exp_dev:] = counts
    masks[me] = mask_out[3]

    def mask_copy(i):
        return remote(mask_out.at[i], masks.at[me], m_send.at[i], m_recv.at[i], peers[i])

    for i in range(3):
        mask_copy(i).start()
    for k in range(1, len(X_CHUNKS)):
        x_far(k).start()
    lax.fori_loop(2, pairs, w1_start, 0)
    for e in range(W2_RING):
        w2_copy(e).start()

    row_id = lax.broadcasted_iota(jnp.int32, (tok, tok), 0)
    col_id = lax.broadcasted_iota(jnp.int32, (tok, tok), 1)
    lower = jnp.where(col_id < row_id, 1.0, 0.0).astype(bf16)
    upper = jnp.where(row_id < col_id, 1.0, 0.0).astype(bf16)
    before = jnp.dot(lower, chosen.astype(bf16), preferred_element_type=f32)
    total = jnp.sum(jnp.exp(logits - top1), axis=1, keepdims=True)
    gates[0] = jnp.broadcast_to(1.0 / total, (tok, 128))
    gates[1] = jnp.broadcast_to(jnp.exp(top2 - top1) / total, (tok, 128))
    mix[...] = jnp.zeros_like(mix)

    slot_id = lax.broadcasted_iota(jnp.int32, (exp_dev, SLOTS, tok), 1).astype(f32)

    def picks(dev):
        m = masks[dev, :exp_dev, :]
        pos = jnp.dot(m, upper, preferred_element_type=f32)
        pos = jnp.where(m.astype(f32) > 0.5, pos, -1.0)
        hot = jnp.where(pos[:, None, :] == slot_id, 1.0, 0.0).reshape(exp_dev * SLOTS, tok).astype(bf16)
        pick_in[dev] = hot

    def gather(dev, first, width):
        cols = slice(first, first + width)
        rows = jnp.dot(pick_in[dev], x_all[x_block(dev), cols], preferred_element_type=f32).astype(bf16)
        rows_in[:, pl.ds(pl.multiple_of(dev * row16, row16), row16), cols] = rows.reshape(pairs, row16, width)

    picks(me)
    own.wait()
    for j in range(0, d_model, 512):
        gather(me, j, 512)
    remote(mask_out.at[2], masks.at[partner], m_send.at[2], m_recv.at[2], partner).wait_recv()
    picks(partner)
    x_near.wait_recv()
    for j in range(0, d_model, 512):
        gather(partner, j, 512)
    for i in range(2):
        remote(mask_out.at[i], masks.at[peers[i]], m_send.at[i], m_recv.at[i], peers[i]).wait_recv()
        picks(peers[i])

    def pass_on(k):
        x_far(k).wait_recv()
        x_fwd(k).start()

    def gather_far(k):
        gather(xn, *X_CHUNKS[k])
        x_fwd(k).wait_recv()
        gather(diag, *X_CHUNKS[k])

    pass_on(0)

    offset = jnp.zeros((1, experts), f32)
    for d in range(4):
        offset = offset + jnp.where(d < me, 1.0, 0.0) * masks[d, exp_dev:, :experts].astype(f32)[0:1]
    position = before + offset
    lane = lax.broadcasted_iota(jnp.int32, (tok, experts), 1)
    dev_id, exp_id = lane // exp_dev, lane % exp_dev
    base = (((exp_id // 4) * 4 + dev_id) * 4 + exp_id % 4) * SLOTS
    base = base.astype(f32) + before
    slot_lane = lax.broadcasted_iota(jnp.int32, (tok, experts * SLOTS), 1).astype(f32)
    for i, hot in enumerate((is1, is2)):
        pos = jnp.sum(jnp.where(hot, position, 0.0), axis=1, keepdims=True)
        slot = jnp.sum(jnp.where(hot, base, 0.0), axis=1, keepdims=True)
        slot = jnp.where(pos < cap, slot, -1.0)
        pick_out[i * tok:(i + 1) * tok, :] = jnp.where(slot_lane == slot, 1.0, 0.0).astype(bf16)

    def weave(a, b):
        blocks = []
        for d in range(4):
            blocks += [a[d * row16:d * row16 + SLOTS], b[d * row16 + SLOTS:(d + 1) * row16]]
        return jnp.concatenate(blocks, axis=0)

    def first_part(c, q, at=None):
        at = q if at is None else at
        rows = rows_in[q, :, c * part:(c + 1) * part]
        a = jnp.dot(rows, w1_buf[at, 0], preferred_element_type=f32)
        b = jnp.dot(rows, w1_buf[at, 1], preferred_element_type=f32)
        return weave(a, b)

    early = pairs // 4
    for c in range(PARTS):
        pass_on(2 * c + 1)
        gather_far(2 * c)
        if c == PARTS - 1:
            pass_on(2 * c + 2)
            gather_far(2 * c + 1)
            gather_far(2 * c + 2)
            break
        gather_far(2 * c + 1)

        def first_product(g, carry):
            for i in range(UNROLL):
                w1_copy(c, g * UNROLL + i).wait()
            for i in range(UNROLL):
                q = g * UNROLL + i
                h = first_part(c, q)
                hid[q] = h if c == 0 else hid[q] + h
            for i in range(UNROLL):
                refill(c, g * UNROLL + i)
            return carry

        def refill(c, q):
            if c < PARTS - 3:
                w1_copy(c + 1, q).start()
            elif c == PARTS - 3:
                mid = (q >= early) & (q < 2 * early)
                w1_copy(jnp.where(mid, PARTS - 1, PARTS - 2), jnp.where(mid, q - early, q), q).start()
            else:
                w1_copy(PARTS - 2, q + early, q).start()

        steps = (pairs if c < PARTS - 2 else early) // UNROLL
        lax.fori_loop(0, steps // 2, first_product, 0)
        pass_on(2 * c + 2)
        lax.fori_loop(steps // 2, steps, first_product, 0)

    units = pairs // 2
    whole = pl.ds(0, d_model)

    def z_rows(dev, q):
        return pl.ds(pl.multiple_of((((q // 2) * 4 + dev) * 2 + q % 2) * row16, row16), row16)

    def z_copy(i, q, c):
        cols = pl.ds(*Z_COLS[c])
        src = z_out.at[q, pl.ds(pl.multiple_of(peers[i] * row16, row16), row16), cols]
        return remote(src, z_in.at[z_rows(me, q), cols], z_send.at[i], z_recv.at[i, z_id(q // 2, c)], peers[i])

    def z_id(u, c):
        return u + jnp.where(u == units - 1, c, 0)

    def unit_wait(u, cols, c):
        for i in range(3):
            rows = pl.ds(pl.multiple_of((u * 4 + peers[i]) * 2 * row16, 2 * row16), 2 * row16)
            here = z_in.at[rows, cols]
            remote(here, here, z_send.at[i], z_recv.at[i, z_id(u, c)], peers[i]).wait_recv()

    def send(q, c):
        for i in range(3):
            z_copy(i, q, c).start()

    def combine(first, depth, lo, hi):
        rows = pl.ds(pl.multiple_of(first, 128), depth)
        block = 512
        gate1 = jnp.concatenate([gates[0]] * (block // 128), axis=1)
        gate2 = jnp.concatenate([gates[1]] * (block // 128), axis=1)
        for j in range(lo, hi, block):
            cols = slice(j, j + block)
            back = jnp.dot(pick_out[:, rows], z_in[rows, cols], preferred_element_type=f32)
            mix[:, cols] += gate1 * back[:tok] + gate2 * back[tok:]

    unit = 4 * 2 * row16

    def finish(q, h):
        hidden = jax.nn.gelu(h, approximate=True).astype(bf16)
        for i in range(2):
            w2_copy(2 * q + i).wait()
        mine = pl.ds(pl.multiple_of(me * row16, row16), row16)
        for c, (lo, size) in enumerate(Z_COLS):
            cols = slice(lo, lo + size)
            a = jnp.dot(hidden, w2_buf[(2 * q) % W2_RING, :, cols], preferred_element_type=f32)
            b = jnp.dot(hidden, w2_buf[(2 * q + 1) % W2_RING, :, cols], preferred_element_type=f32)
            z_out[q, :, cols] = weave(a, b).astype(bf16)
            z_in[z_rows(me, q), cols] = z_out[q, mine, cols]
            send(q, c)
        for i in range(2):
            @pl.when(2 * q + i + W2_RING < exp_dev)
            def _():
                w2_copy(2 * q + i + W2_RING).start()

    def units_in(first, count):
        for i in range(count):
            unit_wait(first + i, whole, 0)
        combine(first * unit, count * unit, 0, d_model)

    def early_pair(q, carry):
        w1_copy(PARTS - 1, q, q + early).wait()
        h = hid[q] + first_part(PARTS - 1, q, q + early)
        w1_copy(PARTS - 1, q + early, q + early).start()
        finish(q, h)
        return carry

    def late_pair(q, carry):
        mid = q < 2 * early
        slot_a = jnp.where(mid, q - early, q)
        slot_b = jnp.where(mid, q, q - 2 * early)
        w1_copy(PARTS - 2, q, slot_a).wait()
        h = hid[q] + first_part(PARTS - 2, q, slot_a)
        w1_copy(PARTS - 1, q, slot_b).wait()
        h = h + first_part(PARTS - 1, q, slot_b)

        @pl.when(mid)
        def _():
            w1_copy(PARTS - 1, q + early, slot_a).start()
            w1_copy(PARTS - 1, q + 2 * early, slot_b).start()

        finish(q, h)

        @pl.when((q == 8) | (q == 13))
        def _():
            units_in((q - 8) // 5 * 2, 2)
        return carry

    lax.fori_loop(0, early, early_pair, 0)
    lax.fori_loop(early, pairs, late_pair, 0)

    def later(u, carry):
        units_in(u, 1)
        return carry

    lax.fori_loop(units // 2, units - 1, later, 0)
    block = x_all.at[x_block(me)]
    for i in range(2):
        remote(block, block, x_send.at[i], own_sem.at[2], xn).wait_send()
    x_near.wait_send()
    for i in range(3):
        mask_copy(i).wait_send()

    def out_copy(c):
        cols = pl.ds(*Z_COLS[c])
        return pltpu.make_async_copy(x_all.at[x_block(me), cols], out_hbm.at[:, cols], own_sem.at[c])

    for c, (lo, size) in enumerate(Z_COLS):
        unit_wait(units - 1, pl.ds(lo, size), c)
        combine((units - 1) * unit, unit, lo, lo + size)
        cols = pl.ds(lo, size)
        x_all[x_block(me), cols] = (x_all[x_block(me), cols].astype(f32) + mix[:, cols]).astype(bf16)
        out_copy(c).start()
    for i in range(3):
        remote(block, block, z_send.at[i], own_sem.at[2], peers[i]).wait_send()
    for c in range(len(Z_COLS)):
        out_copy(c).wait()


def copy_kernel(src, dst, buf, sem):
    rows = buf.shape[0] // COPY_CHUNKS
    block = [pl.ds(i * rows, rows) for i in range(COPY_CHUNKS)]
    load = [pltpu.make_async_copy(src.at[b], buf.at[b], sem.at[0, i]) for i, b in enumerate(block)]
    store = [pltpu.make_async_copy(buf.at[b], dst.at[b], sem.at[1, i]) for i, b in enumerate(block)]
    for c in load:
        c.start()
    for a, b in zip(load, store):
        a.wait()
        b.start()
    for c in store:
        c.wait()


def solution(mesh):
    group = mesh.shape["ep"]
    row_spec = P(("dp", "ep"), None)
    expert_spec = P("ep", None, None)

    def local_step(x_rows, logits, w_in, w_out):
        tok, d_model = x_rows.shape
        experts = logits.shape[1]
        exp_dev, _, d_ff = w_in.shape
        cap = 2 * tok * group // experts
        cfg = (tok, d_model, d_ff, experts, exp_dev, cap)
        bf16 = jnp.bfloat16
        hbm = pl.BlockSpec(memory_space=pl.ANY)
        f32 = jnp.float32
        dma = pltpu.SemaphoreType.DMA
        y = pl.pallas_call(
            functools.partial(moe_kernel, cfg),
            name="moe",
            out_shape=jax.ShapeDtypeStruct((tok, d_model), bf16),
            in_specs=[hbm, hbm, hbm, hbm],
            out_specs=hbm,
            scratch_shapes=[
                pltpu.VMEM((tok, experts), f32),
                pltpu.VMEM((group * tok, d_model), bf16),
                pltpu.VMEM((experts, tok), bf16),
                pltpu.VMEM((group, exp_dev + 8, tok), bf16),
                pltpu.VMEM((group, exp_dev + 8, tok), bf16),
                pltpu.VMEM((exp_dev // 2, group * 2 * SLOTS, d_model), bf16),
                pltpu.VMEM((exp_dev // 2, group * 2 * SLOTS, d_ff), f32),
                pltpu.VMEM((exp_dev // 2, group * 2 * SLOTS, d_model), bf16),
                pltpu.VMEM((experts * SLOTS, d_model), bf16),
                pltpu.VMEM((tok, d_model), f32),
                pltpu.VMEM((2, tok, 128), f32),
                pltpu.VMEM((group, exp_dev * SLOTS, tok), bf16),
                pltpu.VMEM((2 * tok, experts * SLOTS), bf16),
                pltpu.VMEM((exp_dev // 2, 2, d_model // PARTS, d_ff), bf16),
                pltpu.VMEM((W2_RING, d_ff, d_model), bf16),
                dma((exp_dev // 2,)), dma((W2_RING,)), dma((3,)),
                dma((3,)), dma((2, len(X_CHUNKS))),
                dma((3,)), dma((3,)),
                dma((3,)), dma((3, exp_dev // 4 + len(Z_COLS) - 1)),
            ],
            compiler_params=pltpu.CompilerParams(
                collective_id=0, has_side_effects=True, vmem_limit_bytes=67_000_000),
        )(x_rows, logits, w_in, w_out)
        return pl.pallas_call(
            copy_kernel,
            name="place",
            out_shape=jax.ShapeDtypeStruct((tok, d_model), bf16),
            in_specs=[hbm],
            out_specs=hbm,
            scratch_shapes=[pltpu.VMEM((tok, d_model), bf16), dma((2, COPY_CHUNKS))],
        )(y)

    return jax.shard_map(local_step, mesh=mesh, in_specs=(row_spec, row_spec, expert_spec, expert_spec),
                         out_specs=row_spec, check_vma=False)
```

```python
import functools

import jax
import jax.numpy as jnp
from jax import lax
from jax.experimental import pallas as pl
from jax.experimental.pallas import tpu as pltpu
from jax.sharding import PartitionSpec as P

MESH = pl.DeviceIdType.MESH
PARTS = 4
W2_RING = 4
UNROLL = 2
SLOTS = 8
Z_COLS = ((0, 512), (512, 1024), (1536, 512))
X_CHUNKS = tuple((i * 256, 256) for i in range(8))
AHEAD = 2


def moe_kernel(cfg, x_hbm, logits_hbm, w1_hbm, w2_hbm, out_ref,
               logits_ref, x_all, slot_tok, pos_all, ahead, mask_out, masks, rows_in, hid, z_out, z_in, mix, gates, pick_in, pick_out,
               w1_buf, w2_buf,
               w1_sem, w2_sem, own_sem, x_send, x_recv, m_send, m_recv, ahead_recv, z_send, z_recv):
    tok, d_model, d_ff, experts, exp_dev, cap = cfg
    me = lax.axis_index("ep")
    core = me % 2
    partner = me + 1 - 2 * core
    xn = (me + 2) % 4
    diag = 3 - me
    peers = (xn, diag, partner)
    bf16, f32 = jnp.bfloat16, jnp.float32
    part = d_model // PARTS
    pairs = exp_dev // 2
    row16 = 2 * SLOTS

    def remote(src, dst, send, recv, dev):
        return pltpu.make_async_remote_copy(src_ref=src, dst_ref=dst, send_sem=send, recv_sem=recv,
                                            device_id={"ep": dev}, device_id_type=MESH)

    barrier = pltpu.get_barrier_semaphore()
    for peer in peers:
        pl.semaphore_signal(barrier, inc=1, device_id={"ep": peer}, device_id_type=MESH)
    own = pltpu.make_async_copy(x_hbm, x_all.at[pl.ds(pl.multiple_of(me * tok, tok), tok)], own_sem.at[0])
    own.start()
    get_logits = pltpu.make_async_copy(logits_hbm, logits_ref, own_sem.at[1])
    get_logits.start()

    def w1_copy(c, q, to=None):
        to = q if to is None else to
        rows = pl.ds(pl.multiple_of(c * part, part), part)
        return pltpu.make_async_copy(w1_hbm.at[pl.ds(2 * q, 2), rows], w1_buf.at[to], w1_sem.at[to])

    def w2_copy(e):
        return pltpu.make_async_copy(w2_hbm.at[e], w2_buf.at[e % W2_RING], w2_sem.at[e % W2_RING])

    def w1_start(q, carry):
        w1_copy(0, q).start()
        return carry

    lax.fori_loop(0, 2, w1_start, 0)

    def x_block(dev):
        return pl.ds(pl.multiple_of(dev * tok, tok), tok)

    def x_far(k):
        cols = pl.ds(*X_CHUNKS[k])
        mine = x_all.at[x_block(me), cols]
        return remote(mine, mine, x_send, x_recv.at[0, k], xn)

    def x_fwd(k):
        here = x_all.at[x_block(xn), pl.ds(*X_CHUNKS[k])]
        return remote(here, here, x_send, x_recv.at[1, k], partner)

    block = x_all.at[x_block(me)]
    x_near = remote(block, block, x_send, own_sem.at[2], partner)
    pl.semaphore_wait(barrier, 3)
    own.wait()
    x_far(0).start()
    x_near.start()

    get_logits.wait()
    logits = logits_ref[...]
    top1 = jnp.max(logits, axis=1, keepdims=True)
    is1 = logits == top1
    rest = jnp.where(is1, -jnp.inf, logits)
    top2 = jnp.max(rest, axis=1, keepdims=True)
    is2 = rest == top2
    chosen = jnp.where(is1 | is2, 1.0, 0.0)
    row_id = lax.broadcasted_iota(jnp.int32, (tok, tok), 0)
    col_id = lax.broadcasted_iota(jnp.int32, (tok, tok), 1)
    upper = jnp.where(row_id < col_id, 1.0, 0.0).astype(bf16)
    chosen_t = chosen.T
    pos = jnp.dot(chosen_t.astype(bf16), upper, preferred_element_type=f32)
    pos = jnp.where(chosen_t > 0.5, pos, -1.0)
    slot_id = lax.broadcasted_iota(jnp.int32, (experts, SLOTS, tok), 1).astype(f32)
    hot = jnp.where(pos[:, None, :] == slot_id, 1.0, 0.0).reshape(experts * SLOTS, tok).astype(bf16)
    tok_id = (lax.broadcasted_iota(jnp.int32, (8, tok), 1) + 1).astype(f32).astype(bf16)
    slot_tok[...] = lax.dot_general(tok_id, hot, (((1,), (1,)), ((), ())), preferred_element_type=f32).astype(bf16)
    counts = jnp.sum(chosen, axis=0, keepdims=True)
    counts = jnp.broadcast_to(jnp.concatenate([counts] * (tok // experts), axis=1), (8, tok))
    top_row = lax.broadcasted_iota(jnp.int32, (8, tok), 0) == 0
    mine_slots = exp_dev * SLOTS
    for i, dev in enumerate(peers + (me,)):
        lanes = pl.ds(pl.multiple_of(dev * mine_slots, mine_slots), mine_slots)
        mask_out[i] = jnp.where(top_row, slot_tok[:, lanes].astype(f32), counts).astype(bf16)
    masks[me] = mask_out[3]

    def mask_copy(i):
        return remote(mask_out.at[i], masks.at[me], m_send.at[0], m_recv.at[i], peers[i])

    for i in range(3):
        mask_copy(i).start()
    for k in range(1, len(X_CHUNKS) - 1):
        x_far(k).start()

    last = len(X_CHUNKS) - 1
    last_cols = pl.ds(*X_CHUNKS[last])

    def ahead_copy(i, dev):
        dst = rows_in.at[pl.ds(0, AHEAD), pl.ds(pl.multiple_of(dev * row16, row16), row16), last_cols]
        return remote(ahead.at[i], dst, m_send.at[1], ahead_recv.at[i], peers[i])

    pos_all[...] = pos
    for i in range(2):
        few = pos_all[pl.ds(pl.multiple_of(peers[i] * exp_dev, exp_dev), 8), :][:2 * AHEAD]
        few_id = lax.broadcasted_iota(jnp.int32, (2 * AHEAD, SLOTS, tok), 1).astype(f32)
        few = jnp.where(few[:, None, :] == few_id, 1.0, 0.0).reshape(2 * AHEAD * SLOTS, tok).astype(bf16)
        rows = jnp.dot(few, x_all[x_block(me), last_cols], preferred_element_type=f32)
        ahead[i] = rows.astype(bf16).reshape(AHEAD, row16, rows.shape[1])
    for i in range(2):
        ahead_copy(i, me).start()
    x_far(last).start()
    lax.fori_loop(2, pairs, w1_start, 0)
    for e in range(W2_RING):
        w2_copy(e).start()

    lower = jnp.where(col_id < row_id, 1.0, 0.0).astype(bf16)
    before = jnp.dot(lower, chosen.astype(bf16), preferred_element_type=f32)
    total = jnp.sum(jnp.exp(logits - top1), axis=1, keepdims=True)
    gates[0] = jnp.broadcast_to(1.0 / total, (tok, 128))
    gates[1] = jnp.broadcast_to(jnp.exp(top2 - top1) / total, (tok, 128))
    mix[...] = jnp.zeros_like(mix)

    tok_row = (row_id + 1).astype(f32)

    def picks(dev):
        hot = jnp.where(tok_row == masks[dev, 0:1, :].astype(f32), 1.0, 0.0)
        pick_in[dev] = hot.T.astype(bf16)

    def gather(dev, first, width, lo=0):
        cols = slice(first, first + width)
        rows = jnp.dot(pick_in[dev], x_all[x_block(dev), cols], preferred_element_type=f32).astype(bf16)
        rows = rows.reshape(pairs, row16, width)[lo:]
        rows_in[lo:, pl.ds(pl.multiple_of(dev * row16, row16), row16), cols] = rows

    picks(me)
    for j in range(0, d_model, 512):
        gather(me, j, 512)
    remote(mask_out.at[2], masks.at[partner], m_send.at[0], m_recv.at[2], partner).wait_recv()
    picks(partner)
    x_near.wait_recv()
    for j in range(0, d_model, 512):
        gather(partner, j, 512)
    for i in range(2):
        remote(mask_out.at[i], masks.at[peers[i]], m_send.at[0], m_recv.at[i], peers[i]).wait_recv()
        picks(peers[i])

    def pass_on(k):
        x_far(k).wait_recv()
        x_fwd(k).start()

    def gather_far(k, lo=0):
        gather(xn, *X_CHUNKS[k], lo)
        x_fwd(k).wait_recv()
        gather(diag, *X_CHUNKS[k], lo)

    pass_on(0)

    offset = jnp.zeros((1, experts), f32)
    for d in range(4):
        offset = offset + jnp.where(d < me, 1.0, 0.0) * masks[d, :, :experts].astype(f32)[1:2]
    position = before + offset
    lane = lax.broadcasted_iota(jnp.int32, (tok, experts), 1)
    dev_id, exp_id = lane // exp_dev, lane % exp_dev
    base = (((exp_id // 4) * 4 + dev_id) * 4 + exp_id % 4) * SLOTS
    base = base.astype(f32) + before
    slot_lane = lax.broadcasted_iota(jnp.int32, (tok, experts * SLOTS), 1).astype(f32)
    for i, hot in enumerate((is1, is2)):
        pos = jnp.sum(jnp.where(hot, position, 0.0), axis=1, keepdims=True)
        slot = jnp.sum(jnp.where(hot, base, 0.0), axis=1, keepdims=True)
        slot = jnp.where(pos < cap, slot, -1.0)
        pick_out[i * tok:(i + 1) * tok, :] = jnp.where(slot_lane == slot, 1.0, 0.0).astype(bf16)

    def weave(a, b):
        blocks = []
        for d in range(4):
            blocks += [a[d * row16:d * row16 + SLOTS], b[d * row16 + SLOTS:(d + 1) * row16]]
        return jnp.concatenate(blocks, axis=0)

    def first_part(c, q, at=None):
        at = q if at is None else at
        rows = rows_in[q, :, c * part:(c + 1) * part]
        a = jnp.dot(rows, w1_buf[at, 0], preferred_element_type=f32)
        b = jnp.dot(rows, w1_buf[at, 1], preferred_element_type=f32)
        return weave(a, b)

    early = AHEAD
    for c in range(PARTS):
        if c == PARTS - 1:
            gather_far(2 * c)
            for i in range(2):
                ahead_copy(i, peers[i]).wait_recv()
            break
        if c == 0:
            pass_on(1)
        gather_far(2 * c)
        gather_far(2 * c + 1)
        if c == PARTS - 2:
            pass_on(2 * c + 2)

        def first_product(g, carry):
            for i in range(UNROLL):
                w1_copy(c, g * UNROLL + i).wait()
            for i in range(UNROLL):
                q = g * UNROLL + i
                h = first_part(c, q)
                hid[q] = h if c == 0 else hid[q] + h
            for i in range(UNROLL):
                refill(c, g * UNROLL + i)
            return carry

        def refill(c, q):
            if c < PARTS - 3:
                w1_copy(c + 1, q).start()
            elif c == PARTS - 3:
                mid = (q >= early) & (q < 2 * early)
                w1_copy(jnp.where(mid, PARTS - 1, PARTS - 2), jnp.where(mid, q - early, q), q).start()
            else:
                w1_copy(PARTS - 2, q + early, q).start()

        steps = (pairs if c < PARTS - 2 else early) // UNROLL
        if c == PARTS - 2:
            lax.fori_loop(0, steps, first_product, 0)
            continue
        lax.fori_loop(0, steps // 2, first_product, 0)
        pass_on(2 * c + 2)
        lax.fori_loop(steps // 2, steps * 3 // 4, first_product, 0)
        pass_on(2 * c + 3)
        lax.fori_loop(steps * 3 // 4, steps, first_product, 0)

    units = pairs // 2
    whole = pl.ds(0, d_model)

    def z_rows(dev, q):
        return pl.ds(pl.multiple_of((((q // 2) * 4 + dev) * 2 + q % 2) * row16, row16), row16)

    def z_copy(i, q, c):
        cols = pl.ds(*Z_COLS[c])
        src = z_out.at[q, pl.ds(pl.multiple_of(peers[i] * row16, row16), row16), cols]
        return remote(src, z_in.at[z_rows(me, q), cols], z_send, z_recv.at[z_id(q // 2, c)], peers[i])

    def z_id(u, c):
        return u + jnp.where(u == units - 1, c, 0)

    def unit_wait(u, cols, c):
        here = z_in.at[pl.ds(0, 6 * row16), cols]
        remote(here, here, z_send, z_recv.at[z_id(u, c)], xn).wait_recv()

    def send(q, c):
        for i in range(3):
            z_copy(i, q, c).start()

    def combine(first, depth, lo, hi):
        rows = pl.ds(pl.multiple_of(first, 128), depth)
        block = 512
        gate1 = jnp.concatenate([gates[0]] * (block // 128), axis=1)
        gate2 = jnp.concatenate([gates[1]] * (block // 128), axis=1)
        for j in range(lo, hi, block):
            cols = slice(j, j + block)
            back = jnp.dot(pick_out[:, rows], z_in[rows, cols], preferred_element_type=f32)
            mix[:, cols] += gate1 * back[:tok] + gate2 * back[tok:]

    unit = 4 * 2 * row16

    def finish(q, h):
        hidden = jax.nn.gelu(h, approximate=True).astype(bf16)
        for i in range(2):
            w2_copy(2 * q + i).wait()
        mine = pl.ds(pl.multiple_of(me * row16, row16), row16)
        for c, (lo, size) in enumerate(Z_COLS):
            cols = slice(lo, lo + size)
            a = jnp.dot(hidden, w2_buf[(2 * q) % W2_RING, :, cols], preferred_element_type=f32)
            b = jnp.dot(hidden, w2_buf[(2 * q + 1) % W2_RING, :, cols], preferred_element_type=f32)
            z_out[q, :, cols] = weave(a, b).astype(bf16)
            z_in[z_rows(me, q), cols] = z_out[q, mine, cols]
            send(q, c)
        for i in range(2):
            @pl.when(2 * q + i + W2_RING < exp_dev)
            def _():
                w2_copy(2 * q + i + W2_RING).start()

    def units_in(first, count):
        for i in range(count):
            unit_wait(first + i, whole, 0)
        combine(first * unit, count * unit, 0, d_model)

    def early_pair(q, carry):
        w1_copy(PARTS - 1, q, q + early).wait()
        h = hid[q] + first_part(PARTS - 1, q, q + early)
        w1_copy(PARTS - 1, q + early, q + early).start()
        finish(q, h)

        @pl.when(q == AHEAD - 2)
        def _():
            pass_on(last)

        @pl.when(q == AHEAD - 1)
        def _():
            gather_far(last, AHEAD)
        return carry

    def late_pair(q, carry):
        mid = q < 2 * early
        slot_a = jnp.where(mid, q - early, q)
        slot_b = jnp.where(mid, q, q - 2 * early)
        w1_copy(PARTS - 2, q, slot_a).wait()
        h = hid[q] + first_part(PARTS - 2, q, slot_a)
        w1_copy(PARTS - 1, q, slot_b).wait()
        h = h + first_part(PARTS - 1, q, slot_b)

        @pl.when(mid)
        def _():
            w1_copy(PARTS - 1, q + early, slot_a).start()
            w1_copy(PARTS - 1, q + 2 * early, slot_b).start()

        @pl.when((q >= 2 * early) & (q + 2 * early < pairs))
        def _():
            w1_copy(PARTS - 1, q + 2 * early, slot_a).start()

        finish(q, h)

        @pl.when((q == 8) | (q == 13))
        def _():
            units_in((q - 8) // 5 * 2, 2)
        return carry

    lax.fori_loop(0, early, early_pair, 0)
    lax.fori_loop(early, pairs, late_pair, 0)

    def later(u, carry):
        units_in(u, 1)
        return carry

    lax.fori_loop(units // 2, units - 1, later, 0)
    three = x_all.at[pl.ds(0, 3 * tok)]
    remote(three, three, x_send, own_sem.at[2], xn).wait_send()
    remote(mask_out.at[pl.ds(0, 3)], mask_out.at[pl.ds(0, 3)], m_send.at[0], own_sem.at[2], xn).wait_send()
    remote(ahead, ahead, m_send.at[1], own_sem.at[2], xn).wait_send()

    for c, (lo, size) in enumerate(Z_COLS):
        unit_wait(units - 1, pl.ds(lo, size), c)
        combine((units - 1) * unit, unit, lo, lo + size)
        cols = pl.ds(lo, size)
        out_ref[:, cols] = (x_all[x_block(me), cols].astype(f32) + mix[:, cols]).astype(bf16)
    remote(three, three, z_send, own_sem.at[2], xn).wait_send()


def solution(mesh):
    group = mesh.shape["ep"]
    row_spec = P(("dp", "ep"), None)
    expert_spec = P("ep", None, None)

    def local_step(x_rows, logits, w_in, w_out):
        tok, d_model = x_rows.shape
        experts = logits.shape[1]
        exp_dev, _, d_ff = w_in.shape
        cap = 2 * tok * group // experts
        cfg = (tok, d_model, d_ff, experts, exp_dev, cap)
        bf16 = jnp.bfloat16
        hbm = pl.BlockSpec(memory_space=pl.ANY)
        f32 = jnp.float32
        dma = pltpu.SemaphoreType.DMA
        return pl.pallas_call(
            functools.partial(moe_kernel, cfg),
            name="moe",
            out_shape=pltpu.VMEM((tok, d_model), bf16),
            in_specs=[hbm, hbm, hbm, hbm],
            out_specs=pl.BlockSpec(memory_space=pltpu.VMEM),
            scratch_shapes=[
                pltpu.VMEM((tok, experts), f32),
                pltpu.VMEM((group * tok, d_model), bf16),
                pltpu.VMEM((8, experts * SLOTS), bf16),
                pltpu.VMEM((experts, tok), f32),
                pltpu.VMEM((2, AHEAD, 2 * SLOTS, X_CHUNKS[-1][1]), bf16),
                pltpu.VMEM((group, 8, tok), bf16),
                pltpu.VMEM((group, 8, tok), bf16),
                pltpu.VMEM((exp_dev // 2, group * 2 * SLOTS, d_model), bf16),
                pltpu.VMEM((exp_dev // 2, group * 2 * SLOTS, d_ff), f32),
                pltpu.VMEM((exp_dev // 2, group * 2 * SLOTS, d_model), bf16),
                pltpu.VMEM((experts * SLOTS, d_model), bf16),
                pltpu.VMEM((tok, d_model), f32),
                pltpu.VMEM((2, tok, 128), f32),
                pltpu.VMEM((group, exp_dev * SLOTS, tok), bf16),
                pltpu.VMEM((2 * tok, experts * SLOTS), bf16),
                pltpu.VMEM((exp_dev // 2, 2, d_model // PARTS, d_ff), bf16),
                pltpu.VMEM((W2_RING, d_ff, d_model), bf16),
                dma((exp_dev // 2,)), dma((W2_RING,)), dma((3,)),
                dma, dma((2, len(X_CHUNKS))),
                dma((2,)), dma((3,)), dma((2,)),
                dma, dma((exp_dev // 4 + len(Z_COLS) - 1,)),
            ],
            compiler_params=pltpu.CompilerParams(
                collective_id=0, has_side_effects=True, vmem_limit_bytes=64_500_000),
        )(x_rows, logits, w_in, w_out)

    return jax.shard_map(local_step, mesh=mesh, in_specs=(row_spec, row_spec, expert_spec, expert_spec),
                         out_specs=row_spec, check_vma=False)
```

```python
import functools

import jax
import jax.numpy as jnp
from jax import lax
from jax.experimental import pallas as pl
from jax.experimental.pallas import tpu as pltpu
from jax.sharding import PartitionSpec as P

MESH = pl.DeviceIdType.MESH
PARTS = 4
W2_RING = 4
UNROLL = 2
SLOTS = 8
Z_COLS = ((0, 512), (512, 1024), (1536, 512))
X_CHUNKS = tuple((i * 256, 256) for i in range(6)) + ((1536, 128), (1664, 384))
PROMPT = 12
DEFER = 8
AHEAD = 2


def moe_kernel(cfg, x_hbm, logits_hbm, w1_hbm, w2_hbm, out_ref,
               logits_ref, x_all, slot_tok, pos_all, ahead, mask_out, masks, rows_in, hid, z_out, z_in, mix, gates, pick_in, pick_out,
               w1_buf, w2_buf,
               w1_sem, w2_sem, own_sem, x_send, x_recv, m_send, m_recv, ahead_recv, z_send, z_recv):
    tok, d_model, d_ff, experts, exp_dev, cap = cfg
    me = lax.axis_index("ep")
    core = me % 2
    partner = me + 1 - 2 * core
    xn = (me + 2) % 4
    diag = 3 - me
    peers = (xn, diag, partner)
    bf16, f32 = jnp.bfloat16, jnp.float32
    part = d_model // PARTS
    pairs = exp_dev // 2
    row16 = 2 * SLOTS

    def remote(src, dst, send, recv, dev):
        return pltpu.make_async_remote_copy(src_ref=src, dst_ref=dst, send_sem=send, recv_sem=recv,
                                            device_id={"ep": dev}, device_id_type=MESH)

    barrier = pltpu.get_barrier_semaphore()
    for peer in peers:
        pl.semaphore_signal(barrier, inc=1, device_id={"ep": peer}, device_id_type=MESH)
    own = pltpu.make_async_copy(x_hbm, x_all.at[pl.ds(pl.multiple_of(me * tok, tok), tok)], own_sem.at[0])
    own.start()
    get_logits = pltpu.make_async_copy(logits_hbm, logits_ref, own_sem.at[1])
    get_logits.start()

    def w1_copy(c, q, to=None):
        to = q if to is None else to
        rows = pl.ds(pl.multiple_of(c * part, part), part)
        return pltpu.make_async_copy(w1_hbm.at[pl.ds(2 * q, 2), rows], w1_buf.at[to], w1_sem.at[to])

    def w2_copy(e):
        return pltpu.make_async_copy(w2_hbm.at[e], w2_buf.at[e % W2_RING], w2_sem.at[e % W2_RING])

    def w1_start(q, carry):
        w1_copy(0, q).start()
        return carry

    lax.fori_loop(0, 2, w1_start, 0)

    def x_block(dev):
        return pl.ds(pl.multiple_of(dev * tok, tok), tok)

    def x_far(k):
        cols = pl.ds(*X_CHUNKS[k])
        mine = x_all.at[x_block(me), cols]
        return remote(mine, mine, x_send, x_recv.at[0, k], xn)

    def x_fwd(k):
        here = x_all.at[x_block(xn), pl.ds(*X_CHUNKS[k])]
        return remote(here, here, x_send, x_recv.at[1, k], partner)

    block = x_all.at[x_block(me)]
    x_near = remote(block, block, x_send, own_sem.at[2], partner)
    pl.semaphore_wait(barrier, 3)
    own.wait()
    x_far(0).start()
    x_near.start()

    get_logits.wait()
    logits = logits_ref[...]
    top1 = jnp.max(logits, axis=1, keepdims=True)
    is1 = logits == top1
    rest = jnp.where(is1, -jnp.inf, logits)
    top2 = jnp.max(rest, axis=1, keepdims=True)
    is2 = rest == top2
    chosen = jnp.where(is1 | is2, 1.0, 0.0)
    row_id = lax.broadcasted_iota(jnp.int32, (tok, tok), 0)
    col_id = lax.broadcasted_iota(jnp.int32, (tok, tok), 1)
    upper = jnp.where(row_id < col_id, 1.0, 0.0).astype(bf16)
    chosen_t = chosen.T
    pos = jnp.dot(chosen_t.astype(bf16), upper, preferred_element_type=f32)
    pos = jnp.where(chosen_t > 0.5, pos, -1.0)
    slot_id = lax.broadcasted_iota(jnp.int32, (experts, SLOTS, tok), 1).astype(f32)
    hot = jnp.where(pos[:, None, :] == slot_id, 1.0, 0.0).reshape(experts * SLOTS, tok).astype(bf16)
    tok_id = (lax.broadcasted_iota(jnp.int32, (8, tok), 1) + 1).astype(f32).astype(bf16)
    slot_tok[...] = lax.dot_general(tok_id, hot, (((1,), (1,)), ((), ())), preferred_element_type=f32).astype(bf16)
    counts = jnp.sum(chosen, axis=0, keepdims=True)
    counts = jnp.broadcast_to(jnp.concatenate([counts] * (tok // experts), axis=1), (8, tok))
    top_row = lax.broadcasted_iota(jnp.int32, (8, tok), 0) == 0
    mine_slots = exp_dev * SLOTS
    for i, dev in enumerate(peers + (me,)):
        lanes = pl.ds(pl.multiple_of(dev * mine_slots, mine_slots), mine_slots)
        mask_out[i] = jnp.where(top_row, slot_tok[:, lanes].astype(f32), counts).astype(bf16)
    masks[me] = mask_out[3]

    def mask_copy(i):
        return remote(mask_out.at[i], masks.at[me], m_send.at[0], m_recv.at[i], peers[i])

    for i in range(3):
        mask_copy(i).start()
    for k in range(1, len(X_CHUNKS) - 1):
        x_far(k).start()

    last = len(X_CHUNKS) - 1
    last_cols = pl.ds(*X_CHUNKS[last])

    def ahead_copy(i, dev):
        dst = rows_in.at[pl.ds(0, AHEAD), pl.ds(pl.multiple_of(dev * row16, row16), row16), last_cols]
        return remote(ahead.at[i], dst, m_send.at[1], ahead_recv.at[i], peers[i])

    pos_all[...] = pos
    for i in range(2):
        few = pos_all[pl.ds(pl.multiple_of(peers[i] * exp_dev, exp_dev), 8), :][:2 * AHEAD]
        few_id = lax.broadcasted_iota(jnp.int32, (2 * AHEAD, SLOTS, tok), 1).astype(f32)
        few = jnp.where(few[:, None, :] == few_id, 1.0, 0.0).reshape(2 * AHEAD * SLOTS, tok).astype(bf16)
        rows = jnp.dot(few, x_all[x_block(me), last_cols], preferred_element_type=f32)
        ahead[i] = rows.astype(bf16).reshape(AHEAD, row16, rows.shape[1])
    for i in range(2):
        ahead_copy(i, me).start()
    x_far(last).start()
    lax.fori_loop(2, pairs, w1_start, 0)
    for e in range(W2_RING):
        w2_copy(e).start()

    lower = jnp.where(col_id < row_id, 1.0, 0.0).astype(bf16)
    before = jnp.dot(lower, chosen.astype(bf16), preferred_element_type=f32)
    total = jnp.sum(jnp.exp(logits - top1), axis=1, keepdims=True)
    gates[0] = jnp.broadcast_to(1.0 / total, (tok, 128))
    gates[1] = jnp.broadcast_to(jnp.exp(top2 - top1) / total, (tok, 128))
    mix[...] = jnp.zeros_like(mix)

    tok_row = (row_id + 1).astype(f32)

    def picks(dev):
        hot = jnp.where(tok_row == masks[dev, 0:1, :].astype(f32), 1.0, 0.0)
        pick_in[dev] = hot.T.astype(bf16)

    def gather(dev, first, width, lo=0):
        cols = slice(first, first + width)
        rows = jnp.dot(pick_in[dev], x_all[x_block(dev), cols], preferred_element_type=f32).astype(bf16)
        rows = rows.reshape(pairs, row16, width)[lo:]
        rows_in[lo:, pl.ds(pl.multiple_of(dev * row16, row16), row16), cols] = rows

    picks(me)
    for j in range(0, d_model, 512):
        gather(me, j, 512)
    remote(mask_out.at[2], masks.at[partner], m_send.at[0], m_recv.at[2], partner).wait_recv()
    picks(partner)
    x_near.wait_recv()
    for j in range(0, d_model, 512):
        gather(partner, j, 512)
    for i in range(2):
        remote(mask_out.at[i], masks.at[peers[i]], m_send.at[0], m_recv.at[i], peers[i]).wait_recv()
        picks(peers[i])

    def pass_on(k):
        x_far(k).wait_recv()
        x_fwd(k).start()

    def gather_far(k, lo=0):
        gather(xn, *X_CHUNKS[k], lo)
        x_fwd(k).wait_recv()
        gather(diag, *X_CHUNKS[k], lo)

    pass_on(0)

    offset = jnp.zeros((1, experts), f32)
    for d in range(4):
        offset = offset + jnp.where(d < me, 1.0, 0.0) * masks[d, :, :experts].astype(f32)[1:2]
    position = before + offset
    lane = lax.broadcasted_iota(jnp.int32, (tok, experts), 1)
    dev_id, exp_id = lane // exp_dev, lane % exp_dev
    base = (((exp_id // 4) * 4 + dev_id) * 4 + exp_id % 4) * SLOTS
    base = base.astype(f32) + before
    slot_lane = lax.broadcasted_iota(jnp.int32, (tok, experts * SLOTS), 1).astype(f32)
    for i, hot in enumerate((is1, is2)):
        pos = jnp.sum(jnp.where(hot, position, 0.0), axis=1, keepdims=True)
        slot = jnp.sum(jnp.where(hot, base, 0.0), axis=1, keepdims=True)
        slot = jnp.where(pos < cap, slot, -1.0)
        pick_out[i * tok:(i + 1) * tok, :] = jnp.where(slot_lane == slot, 1.0, 0.0).astype(bf16)

    def weave(a, b):
        blocks = []
        for d in range(4):
            blocks += [a[d * row16:d * row16 + SLOTS], b[d * row16 + SLOTS:(d + 1) * row16]]
        return jnp.concatenate(blocks, axis=0)

    def first_part(c, q, at=None):
        at = q if at is None else at
        rows = rows_in[q, :, c * part:(c + 1) * part]
        both = jnp.concatenate([w1_buf[at, 0], w1_buf[at, 1]], axis=1)
        h = jnp.dot(rows, both, preferred_element_type=f32)
        return weave(h[:, :d_ff], h[:, d_ff:])

    early = AHEAD
    for c in range(PARTS):
        if c == PARTS - 1:
            gather_far(2 * c)
            for i in range(2):
                ahead_copy(i, peers[i]).wait_recv()
            break
        if c == 0:
            pass_on(1)
        for k in (2 * c, 2 * c + 1):
            x_fwd(k).wait_recv()
        for dev in (xn, diag):
            gather(dev, c * part, part)
        if c == PARTS - 2:
            pass_on(2 * c + 2)

        def first_product(g, carry):
            for i in range(UNROLL):
                w1_copy(c, g * UNROLL + i).wait()
            for i in range(UNROLL):
                q = g * UNROLL + i
                h = first_part(c, q)
                hid[q] = h if c == 0 else hid[q] + h
            for i in range(UNROLL):
                refill(c, g * UNROLL + i)
            return carry

        def refill(c, q):
            if c < PARTS - 3:
                w1_copy(c + 1, q).start()
            elif c == PARTS - 3:
                mid = (q >= early) & (q < 2 * early)

                @pl.when(q < PROMPT)
                def _():
                    w1_copy(jnp.where(mid, PARTS - 1, PARTS - 2), jnp.where(mid, q - early, q), q).start()
            else:
                w1_copy(PARTS - 2, q + early, q).start()

        steps = (pairs if c < PARTS - 2 else early) // UNROLL
        if c == PARTS - 2:
            lax.fori_loop(0, steps, first_product, 0)
            continue
        lax.fori_loop(0, steps // 2, first_product, 0)
        pass_on(2 * c + 2)
        lax.fori_loop(steps // 2, steps * 7 // 8, first_product, 0)
        pass_on(2 * c + 3)
        lax.fori_loop(steps * 7 // 8, steps, first_product, 0)

    units = pairs // 2
    whole = pl.ds(0, d_model)

    def z_rows(dev, q):
        return pl.ds(pl.multiple_of((((q // 2) * 4 + dev) * 2 + q % 2) * row16, row16), row16)

    def z_copy(i, q, c):
        cols = pl.ds(*Z_COLS[c])
        src = z_out.at[q, pl.ds(pl.multiple_of(peers[i] * row16, row16), row16), cols]
        return remote(src, z_in.at[z_rows(me, q), cols], z_send, z_recv.at[z_id(q // 2, c)], peers[i])

    def z_id(u, c):
        return u + jnp.where(u == units - 1, c, 0)

    def unit_wait(u, cols, c):
        here = z_in.at[pl.ds(0, 6 * row16), cols]
        remote(here, here, z_send, z_recv.at[z_id(u, c)], xn).wait_recv()

    def send(q, c):
        for i in range(3):
            z_copy(i, q, c).start()

    def combine(first, depth, lo, hi):
        rows = pl.ds(pl.multiple_of(first, 128), depth)
        block = 512
        gate1 = jnp.concatenate([gates[0]] * (block // 128), axis=1)
        gate2 = jnp.concatenate([gates[1]] * (block // 128), axis=1)
        for j in range(lo, hi, block):
            cols = slice(j, j + block)
            back = jnp.dot(pick_out[:, rows], z_in[rows, cols], preferred_element_type=f32)
            mix[:, cols] += gate1 * back[:tok] + gate2 * back[tok:]

    unit = 4 * 2 * row16

    def finish(q, h):
        hidden = jax.nn.gelu(h, approximate=True).astype(bf16)
        for i in range(2):
            w2_copy(2 * q + i).wait()
        mine = pl.ds(pl.multiple_of(me * row16, row16), row16)
        for c, (lo, size) in enumerate(Z_COLS):
            cols = slice(lo, lo + size)
            a = jnp.dot(hidden, w2_buf[(2 * q) % W2_RING, :, cols], preferred_element_type=f32)
            b = jnp.dot(hidden, w2_buf[(2 * q + 1) % W2_RING, :, cols], preferred_element_type=f32)
            z_out[q, :, cols] = weave(a, b).astype(bf16)
            z_in[z_rows(me, q), cols] = z_out[q, mine, cols]
            send(q, c)
        for i in range(2):
            @pl.when(2 * q + i + W2_RING < exp_dev)
            def _():
                w2_copy(2 * q + i + W2_RING).start()

    def units_in(first, count):
        for i in range(count):
            unit_wait(first + i, whole, 0)
        combine(first * unit, count * unit, 0, d_model)

    def early_pair(q, carry):
        w1_copy(PARTS - 1, q, q + early).wait()
        h = hid[q] + first_part(PARTS - 1, q, q + early)
        w1_copy(PARTS - 1, q + early, q + early).start()
        finish(q, h)

        @pl.when(q == AHEAD - 2)
        def _():
            pass_on(last)

        @pl.when(q == AHEAD - 1)
        def _():
            gather_far(last, AHEAD)
        return carry

    def late_pair(q, carry):
        mid = q < 2 * early
        slot_a = jnp.where(mid, q - early, q)
        slot_b = jnp.where(mid, q, q - 2 * early)
        w1_copy(PARTS - 2, q, slot_a).wait()

        @pl.when((q + DEFER >= PROMPT) & (q + DEFER < pairs))
        def _():
            w1_copy(PARTS - 2, q + DEFER, q + DEFER).start()

        h = hid[q] + first_part(PARTS - 2, q, slot_a)
        w1_copy(PARTS - 1, q, slot_b).wait()
        h = h + first_part(PARTS - 1, q, slot_b)

        @pl.when(mid)
        def _():
            w1_copy(PARTS - 1, q + early, slot_a).start()
            w1_copy(PARTS - 1, q + 2 * early, slot_b).start()

        @pl.when((q >= 2 * early) & (q + 2 * early < pairs))
        def _():
            w1_copy(PARTS - 1, q + 2 * early, slot_a).start()

        finish(q, h)

        @pl.when((q == 8) | (q == 13))
        def _():
            units_in((q - 8) // 5 * 2, 2)
        return carry

    lax.fori_loop(0, early, early_pair, 0)
    lax.fori_loop(early, pairs, late_pair, 0)

    def later(u, carry):
        units_in(u, 1)
        return carry

    lax.fori_loop(units // 2, units - 1, later, 0)
    three = x_all.at[pl.ds(0, 3 * tok)]
    remote(three, three, x_send, own_sem.at[2], xn).wait_send()
    remote(mask_out.at[pl.ds(0, 3)], mask_out.at[pl.ds(0, 3)], m_send.at[0], own_sem.at[2], xn).wait_send()
    remote(ahead, ahead, m_send.at[1], own_sem.at[2], xn).wait_send()

    for c, (lo, size) in enumerate(Z_COLS):
        unit_wait(units - 1, pl.ds(lo, size), c)
        combine((units - 1) * unit, unit, lo, lo + size)
        cols = pl.ds(lo, size)
        out_ref[:, cols] = (x_all[x_block(me), cols].astype(f32) + mix[:, cols]).astype(bf16)
    remote(three, three, z_send, own_sem.at[2], xn).wait_send()


def solution(mesh):
    group = mesh.shape["ep"]
    row_spec = P(("dp", "ep"), None)
    expert_spec = P("ep", None, None)

    def local_step(x_rows, logits, w_in, w_out):
        tok, d_model = x_rows.shape
        experts = logits.shape[1]
        exp_dev, _, d_ff = w_in.shape
        cap = 2 * tok * group // experts
        cfg = (tok, d_model, d_ff, experts, exp_dev, cap)
        bf16 = jnp.bfloat16
        hbm = pl.BlockSpec(memory_space=pl.ANY)
        f32 = jnp.float32
        dma = pltpu.SemaphoreType.DMA
        return pl.pallas_call(
            functools.partial(moe_kernel, cfg),
            name="moe",
            out_shape=pltpu.VMEM((tok, d_model), bf16),
            in_specs=[hbm, hbm, hbm, hbm],
            out_specs=pl.BlockSpec(memory_space=pltpu.VMEM),
            scratch_shapes=[
                pltpu.VMEM((tok, experts), f32),
                pltpu.VMEM((group * tok, d_model), bf16),
                pltpu.VMEM((8, experts * SLOTS), bf16),
                pltpu.VMEM((experts, tok), f32),
                pltpu.VMEM((2, AHEAD, 2 * SLOTS, X_CHUNKS[-1][1]), bf16),
                pltpu.VMEM((group, 8, tok), bf16),
                pltpu.VMEM((group, 8, tok), bf16),
                pltpu.VMEM((exp_dev // 2, group * 2 * SLOTS, d_model), bf16),
                pltpu.VMEM((exp_dev // 2, group * 2 * SLOTS, d_ff), f32),
                pltpu.VMEM((exp_dev // 2, group * 2 * SLOTS, d_model), bf16),
                pltpu.VMEM((experts * SLOTS, d_model), bf16),
                pltpu.VMEM((tok, d_model), f32),
                pltpu.VMEM((2, tok, 128), f32),
                pltpu.VMEM((group, exp_dev * SLOTS, tok), bf16),
                pltpu.VMEM((2 * tok, experts * SLOTS), bf16),
                pltpu.VMEM((exp_dev // 2, 2, d_model // PARTS, d_ff), bf16),
                pltpu.VMEM((W2_RING, d_ff, d_model), bf16),
                dma((exp_dev // 2,)), dma((W2_RING,)), dma((3,)),
                dma, dma((2, len(X_CHUNKS))),
                dma((2,)), dma((3,)), dma((2,)),
                dma, dma((exp_dev // 4 + len(Z_COLS) - 1,)),
            ],
            compiler_params=pltpu.CompilerParams(
                collective_id=0, has_side_effects=True, vmem_limit_bytes=64_500_000),
        )(x_rows, logits, w_in, w_out)

    return jax.shard_map(local_step, mesh=mesh, in_specs=(row_spec, row_spec, expert_spec, expert_spec),
                         out_specs=row_spec, check_vma=False)
```

```python
import functools

import jax
import jax.numpy as jnp
from jax import lax
from jax.experimental import pallas as pl
from jax.experimental.pallas import tpu as pltpu
from jax.sharding import PartitionSpec as P

MESH = pl.DeviceIdType.MESH
PARTS = 4
W2_RING = 4
UNROLL = 2
SLOTS = 8
Z_COLS = ((0, 512), (512, 1024), (1536, 512))
X_CHUNKS = tuple((i * 256, 256) for i in range(6)) + ((1536, 512),)
PROMPT = 12
DEFER = 8
AHEAD = 2


def moe_kernel(cfg, x_hbm, logits_hbm, w1_hbm, w2_hbm, out_ref,
               logits_ref, x_all, slot_tok, pos_all, ahead, mask_out, masks, rows_in, hid, z_out, z_in, mix, gates, pick_in, pick_out,
               w1_buf, w2_buf,
               w1_sem, w2_sem, own_sem, x_send, x_recv, m_send, m_recv, ahead_recv, z_send, z_recv):
    tok, d_model, d_ff, experts, exp_dev, cap = cfg
    me = lax.axis_index("ep")
    core = me % 2
    partner = me + 1 - 2 * core
    xn = (me + 2) % 4
    diag = 3 - me
    peers = (xn, diag, partner)
    bf16, f32 = jnp.bfloat16, jnp.float32
    part = d_model // PARTS
    pairs = exp_dev // 2
    row16 = 2 * SLOTS

    def remote(src, dst, send, recv, dev):
        return pltpu.make_async_remote_copy(src_ref=src, dst_ref=dst, send_sem=send, recv_sem=recv,
                                            device_id={"ep": dev}, device_id_type=MESH)

    barrier = pltpu.get_barrier_semaphore()
    for peer in peers:
        pl.semaphore_signal(barrier, inc=1, device_id={"ep": peer}, device_id_type=MESH)
    own = pltpu.make_async_copy(x_hbm, x_all.at[pl.ds(pl.multiple_of(me * tok, tok), tok)], own_sem.at[0])
    own.start()
    get_logits = pltpu.make_async_copy(logits_hbm, logits_ref, own_sem.at[1])
    get_logits.start()

    def w1_copy(c, q, to=None):
        to = q if to is None else to
        rows = pl.ds(pl.multiple_of(c * part, part), part)
        return pltpu.make_async_copy(w1_hbm.at[pl.ds(2 * q, 2), rows], w1_buf.at[to], w1_sem.at[to])

    def w2_copy(e):
        return pltpu.make_async_copy(w2_hbm.at[e], w2_buf.at[e % W2_RING], w2_sem.at[e % W2_RING])

    def w1_start(q, carry):
        w1_copy(0, q).start()
        return carry

    lax.fori_loop(0, 2, w1_start, 0)

    def x_block(dev):
        return pl.ds(pl.multiple_of(dev * tok, tok), tok)

    def x_far(k):
        cols = pl.ds(*X_CHUNKS[k])
        mine = x_all.at[x_block(me), cols]
        return remote(mine, mine, x_send, x_recv.at[0, k], xn)

    def x_fwd(k):
        here = x_all.at[x_block(xn), pl.ds(*X_CHUNKS[k])]
        return remote(here, here, x_send, x_recv.at[1, k], partner)

    block = x_all.at[x_block(me)]
    x_near = remote(block, block, x_send, own_sem.at[2], partner)
    pl.semaphore_wait(barrier, 3)
    own.wait()
    x_far(0).start()
    x_near.start()

    get_logits.wait()
    logits = logits_ref[...]
    top1 = jnp.max(logits, axis=1, keepdims=True)
    is1 = logits == top1
    rest = jnp.where(is1, -jnp.inf, logits)
    top2 = jnp.max(rest, axis=1, keepdims=True)
    is2 = rest == top2
    chosen = jnp.where(is1 | is2, 1.0, 0.0)
    row_id = lax.broadcasted_iota(jnp.int32, (tok, tok), 0)
    col_id = lax.broadcasted_iota(jnp.int32, (tok, tok), 1)
    upper = jnp.where(row_id < col_id, 1.0, 0.0).astype(bf16)
    chosen_t = chosen.T
    pos = jnp.dot(chosen_t.astype(bf16), upper, preferred_element_type=f32)
    pos = jnp.where(chosen_t > 0.5, pos, -1.0)
    slot_id = lax.broadcasted_iota(jnp.int32, (experts, SLOTS, tok), 1).astype(f32)
    hot = jnp.where(pos[:, None, :] == slot_id, 1.0, 0.0).reshape(experts * SLOTS, tok).astype(bf16)
    tok_id = (lax.broadcasted_iota(jnp.int32, (8, tok), 1) + 1).astype(f32).astype(bf16)
    slot_tok[...] = lax.dot_general(tok_id, hot, (((1,), (1,)), ((), ())), preferred_element_type=f32).astype(bf16)
    counts = jnp.sum(chosen, axis=0, keepdims=True)
    counts = jnp.broadcast_to(jnp.concatenate([counts] * (tok // experts), axis=1), (8, tok))
    top_row = lax.broadcasted_iota(jnp.int32, (8, tok), 0) == 0
    mine_slots = exp_dev * SLOTS
    for i, dev in enumerate(peers + (me,)):
        lanes = pl.ds(pl.multiple_of(dev * mine_slots, mine_slots), mine_slots)
        mask_out[i] = jnp.where(top_row, slot_tok[:, lanes].astype(f32), counts).astype(bf16)
    masks[me] = mask_out[3]

    def mask_copy(i):
        return remote(mask_out.at[i], masks.at[me], m_send.at[0], m_recv.at[i], peers[i])

    for i in range(3):
        mask_copy(i).start()
    for k in range(1, len(X_CHUNKS) - 1):
        x_far(k).start()

    last = len(X_CHUNKS) - 1
    last_cols = pl.ds(*X_CHUNKS[last])

    def ahead_copy(i, dev):
        dst = rows_in.at[pl.ds(0, AHEAD), pl.ds(pl.multiple_of(dev * row16, row16), row16), last_cols]
        return remote(ahead.at[i], dst, m_send.at[1], ahead_recv.at[i], peers[i])

    pos_all[...] = pos
    for i in range(2):
        few = pos_all[pl.ds(pl.multiple_of(peers[i] * exp_dev, exp_dev), 8), :][:2 * AHEAD]
        few_id = lax.broadcasted_iota(jnp.int32, (2 * AHEAD, SLOTS, tok), 1).astype(f32)
        few = jnp.where(few[:, None, :] == few_id, 1.0, 0.0).reshape(2 * AHEAD * SLOTS, tok).astype(bf16)
        rows = jnp.dot(few, x_all[x_block(me), last_cols], preferred_element_type=f32)
        ahead[i] = rows.astype(bf16).reshape(AHEAD, row16, rows.shape[1])
    for i in range(2):
        ahead_copy(i, me).start()
    x_far(last).start()
    lax.fori_loop(2, pairs, w1_start, 0)
    for e in range(W2_RING):
        w2_copy(e).start()

    lower = jnp.where(col_id < row_id, 1.0, 0.0).astype(bf16)
    before = jnp.dot(lower, chosen.astype(bf16), preferred_element_type=f32)
    total = jnp.sum(jnp.exp(logits - top1), axis=1, keepdims=True)
    gates[0] = jnp.broadcast_to(1.0 / total, (tok, 128))
    gates[1] = jnp.broadcast_to(jnp.exp(top2 - top1) / total, (tok, 128))
    mix[...] = jnp.zeros_like(mix)

    tok_row = (row_id + 1).astype(f32)

    def picks(dev):
        hot = jnp.where(tok_row == masks[dev, 0:1, :].astype(f32), 1.0, 0.0)
        pick_in[dev] = hot.T.astype(bf16)

    def gather(dev, first, width, lo=0):
        cols = slice(first, first + width)
        rows = jnp.dot(pick_in[dev], x_all[x_block(dev), cols], preferred_element_type=f32).astype(bf16)
        rows = rows.reshape(pairs, row16, width)[lo:]
        rows_in[lo:, pl.ds(pl.multiple_of(dev * row16, row16), row16), cols] = rows

    picks(me)
    for j in range(0, d_model, 512):
        gather(me, j, 512)
    remote(mask_out.at[2], masks.at[partner], m_send.at[0], m_recv.at[2], partner).wait_recv()
    picks(partner)
    x_near.wait_recv()
    for j in range(0, d_model, 512):
        gather(partner, j, 512)
    for i in range(2):
        remote(mask_out.at[i], masks.at[peers[i]], m_send.at[0], m_recv.at[i], peers[i]).wait_recv()
        picks(peers[i])

    def pass_on(k):
        x_far(k).wait_recv()
        x_fwd(k).start()

    def gather_far(k, lo=0):
        gather(xn, *X_CHUNKS[k], lo)
        x_fwd(k).wait_recv()
        gather(diag, *X_CHUNKS[k], lo)

    pass_on(0)

    offset = jnp.zeros((1, experts), f32)
    for d in range(4):
        offset = offset + jnp.where(d < me, 1.0, 0.0) * masks[d, :, :experts].astype(f32)[1:2]
    position = before + offset
    lane = lax.broadcasted_iota(jnp.int32, (tok, experts), 1)
    dev_id, exp_id = lane // exp_dev, lane % exp_dev
    base = (((exp_id // 4) * 4 + dev_id) * 4 + exp_id % 4) * SLOTS
    base = base.astype(f32) + before
    slot_lane = lax.broadcasted_iota(jnp.int32, (tok, experts * SLOTS), 1).astype(f32)
    for i, hot in enumerate((is1, is2)):
        pos = jnp.sum(jnp.where(hot, position, 0.0), axis=1, keepdims=True)
        slot = jnp.sum(jnp.where(hot, base, 0.0), axis=1, keepdims=True)
        slot = jnp.where(pos < cap, slot, -1.0)
        pick_out[i * tok:(i + 1) * tok, :] = jnp.where(slot_lane == slot, 1.0, 0.0).astype(bf16)

    def weave(a, b):
        blocks = []
        for d in range(4):
            blocks += [a[d * row16:d * row16 + SLOTS], b[d * row16 + SLOTS:(d + 1) * row16]]
        return jnp.concatenate(blocks, axis=0)

    def first_part(c, q, at=None):
        at = q if at is None else at
        rows = rows_in[q, :, c * part:(c + 1) * part]
        both = jnp.concatenate([w1_buf[at, 0], w1_buf[at, 1]], axis=1)
        h = jnp.dot(rows, both, preferred_element_type=f32)
        return weave(h[:, :d_ff], h[:, d_ff:])

    early = AHEAD
    for c in range(PARTS):
        if c == PARTS - 1:
            for i in range(2):
                ahead_copy(i, peers[i]).wait_recv()
            break
        if c == 0:
            pass_on(1)
        for k in (2 * c, 2 * c + 1):
            x_fwd(k).wait_recv()
        for dev in (xn, diag):
            gather(dev, c * part, part)
        def first_product(g, carry):
            for i in range(UNROLL):
                w1_copy(c, g * UNROLL + i).wait()
            for i in range(UNROLL):
                q = g * UNROLL + i
                h = first_part(c, q)
                hid[q] = h if c == 0 else hid[q] + h
            for i in range(UNROLL):
                refill(c, g * UNROLL + i)
            return carry

        def refill(c, q):
            if c < PARTS - 3:
                w1_copy(c + 1, q).start()
            elif c == PARTS - 3:
                mid = (q >= early) & (q < 2 * early)

                @pl.when(q < PROMPT)
                def _():
                    w1_copy(jnp.where(mid, PARTS - 1, PARTS - 2), jnp.where(mid, q - early, q), q).start()
            else:
                w1_copy(PARTS - 2, q + early, q).start()

        steps = (pairs if c < PARTS - 2 else early) // UNROLL
        if c == PARTS - 2:
            lax.fori_loop(0, steps, first_product, 0)
            continue
        lax.fori_loop(0, steps // 2, first_product, 0)
        pass_on(2 * c + 2)
        lax.fori_loop(steps // 2, steps * 7 // 8, first_product, 0)
        pass_on(2 * c + 3)
        lax.fori_loop(steps * 7 // 8, steps, first_product, 0)

    units = pairs // 2
    whole = pl.ds(0, d_model)

    def z_rows(dev, q):
        return pl.ds(pl.multiple_of((((q // 2) * 4 + dev) * 2 + q % 2) * row16, row16), row16)

    def z_copy(i, q, c):
        cols = pl.ds(*Z_COLS[c])
        src = z_out.at[q, pl.ds(pl.multiple_of(peers[i] * row16, row16), row16), cols]
        return remote(src, z_in.at[z_rows(me, q), cols], z_send, z_recv.at[z_id(q // 2, c)], peers[i])

    def z_id(u, c):
        return u + jnp.where(u == units - 1, c, 0)

    def unit_wait(u, cols, c):
        here = z_in.at[pl.ds(0, 6 * row16), cols]
        remote(here, here, z_send, z_recv.at[z_id(u, c)], xn).wait_recv()

    def send(q, c):
        for i in range(3):
            z_copy(i, q, c).start()

    def combine(first, depth, lo, hi):
        rows = pl.ds(pl.multiple_of(first, 128), depth)
        block = 512
        gate1 = jnp.concatenate([gates[0]] * (block // 128), axis=1)
        gate2 = jnp.concatenate([gates[1]] * (block // 128), axis=1)
        for j in range(lo, hi, block):
            cols = slice(j, j + block)
            back = jnp.dot(pick_out[:, rows], z_in[rows, cols], preferred_element_type=f32)
            mix[:, cols] += gate1 * back[:tok] + gate2 * back[tok:]

    unit = 4 * 2 * row16

    def finish(q, h):
        hidden = jax.nn.gelu(h, approximate=True).astype(bf16)
        for i in range(2):
            w2_copy(2 * q + i).wait()
        mine = pl.ds(pl.multiple_of(me * row16, row16), row16)
        for c, (lo, size) in enumerate(Z_COLS):
            cols = slice(lo, lo + size)
            a = jnp.dot(hidden, w2_buf[(2 * q) % W2_RING, :, cols], preferred_element_type=f32)
            b = jnp.dot(hidden, w2_buf[(2 * q + 1) % W2_RING, :, cols], preferred_element_type=f32)
            z_out[q, :, cols] = weave(a, b).astype(bf16)
            z_in[z_rows(me, q), cols] = z_out[q, mine, cols]
            send(q, c)
        for i in range(2):
            @pl.when(2 * q + i + W2_RING < exp_dev)
            def _():
                w2_copy(2 * q + i + W2_RING).start()

    def units_in(first, count):
        for i in range(count):
            unit_wait(first + i, whole, 0)
        combine(first * unit, count * unit, 0, d_model)

    def early_pair(q, carry):
        w1_copy(PARTS - 1, q, q + early).wait()
        h = hid[q] + first_part(PARTS - 1, q, q + early)
        w1_copy(PARTS - 1, q + early, q + early).start()
        finish(q, h)

        @pl.when(q == AHEAD - 1)
        def _():
            pass_on(last)
            gather_far(last, AHEAD)
        return carry

    def late_pair(q, carry):
        mid = q < 2 * early
        slot_a = jnp.where(mid, q - early, q)
        slot_b = jnp.where(mid, q, q - 2 * early)
        w1_copy(PARTS - 2, q, slot_a).wait()

        @pl.when((q + DEFER >= PROMPT) & (q + DEFER < pairs))
        def _():
            w1_copy(PARTS - 2, q + DEFER, q + DEFER).start()

        h = hid[q] + first_part(PARTS - 2, q, slot_a)
        w1_copy(PARTS - 1, q, slot_b).wait()
        h = h + first_part(PARTS - 1, q, slot_b)

        @pl.when(mid)
        def _():
            w1_copy(PARTS - 1, q + early, slot_a).start()
            w1_copy(PARTS - 1, q + 2 * early, slot_b).start()

        @pl.when((q >= 2 * early) & (q + 2 * early < pairs))
        def _():
            w1_copy(PARTS - 1, q + 2 * early, slot_a).start()

        finish(q, h)

        @pl.when((q == 8) | (q == 13))
        def _():
            units_in((q - 8) // 5 * 2, 2)
        return carry

    lax.fori_loop(0, early, early_pair, 0)
    lax.fori_loop(early, pairs, late_pair, 0)

    def later(u, carry):
        units_in(u, 1)
        return carry

    lax.fori_loop(units // 2, units - 1, later, 0)
    three = x_all.at[pl.ds(0, 3 * tok)]
    remote(three, three, x_send, own_sem.at[2], xn).wait_send()
    remote(mask_out.at[pl.ds(0, 3)], mask_out.at[pl.ds(0, 3)], m_send.at[0], own_sem.at[2], xn).wait_send()
    remote(ahead, ahead, m_send.at[1], own_sem.at[2], xn).wait_send()

    for c, (lo, size) in enumerate(Z_COLS):
        unit_wait(units - 1, pl.ds(lo, size), c)
        combine((units - 1) * unit, unit, lo, lo + size)
        cols = pl.ds(lo, size)
        out_ref[:, cols] = (x_all[x_block(me), cols].astype(f32) + mix[:, cols]).astype(bf16)
    remote(three, three, z_send, own_sem.at[2], xn).wait_send()


def solution(mesh):
    group = mesh.shape["ep"]
    row_spec = P(("dp", "ep"), None)
    expert_spec = P("ep", None, None)

    def local_step(x_rows, logits, w_in, w_out):
        tok, d_model = x_rows.shape
        experts = logits.shape[1]
        exp_dev, _, d_ff = w_in.shape
        cap = 2 * tok * group // experts
        cfg = (tok, d_model, d_ff, experts, exp_dev, cap)
        bf16 = jnp.bfloat16
        hbm = pl.BlockSpec(memory_space=pl.ANY)
        f32 = jnp.float32
        dma = pltpu.SemaphoreType.DMA
        return pl.pallas_call(
            functools.partial(moe_kernel, cfg),
            name="moe",
            out_shape=pltpu.VMEM((tok, d_model), bf16),
            in_specs=[hbm, hbm, hbm, hbm],
            out_specs=pl.BlockSpec(memory_space=pltpu.VMEM),
            scratch_shapes=[
                pltpu.VMEM((tok, experts), f32),
                pltpu.VMEM((group * tok, d_model), bf16),
                pltpu.VMEM((8, experts * SLOTS), bf16),
                pltpu.VMEM((experts, tok), f32),
                pltpu.VMEM((2, AHEAD, 2 * SLOTS, X_CHUNKS[-1][1]), bf16),
                pltpu.VMEM((group, 8, tok), bf16),
                pltpu.VMEM((group, 8, tok), bf16),
                pltpu.VMEM((exp_dev // 2, group * 2 * SLOTS, d_model), bf16),
                pltpu.VMEM((exp_dev // 2, group * 2 * SLOTS, d_ff), f32),
                pltpu.VMEM((exp_dev // 2, group * 2 * SLOTS, d_model), bf16),
                pltpu.VMEM((experts * SLOTS, d_model), bf16),
                pltpu.VMEM((tok, d_model), f32),
                pltpu.VMEM((2, tok, 128), f32),
                pltpu.VMEM((group, exp_dev * SLOTS, tok), bf16),
                pltpu.VMEM((2 * tok, experts * SLOTS), bf16),
                pltpu.VMEM((exp_dev // 2, 2, d_model // PARTS, d_ff), bf16),
                pltpu.VMEM((W2_RING, d_ff, d_model), bf16),
                dma((exp_dev // 2,)), dma((W2_RING,)), dma((3,)),
                dma, dma((2, len(X_CHUNKS))),
                dma((2,)), dma((3,)), dma((2,)),
                dma, dma((exp_dev // 4 + len(Z_COLS) - 1,)),
            ],
            compiler_params=pltpu.CompilerParams(
                collective_id=0, has_side_effects=True, vmem_limit_bytes=64_500_000),
        )(x_rows, logits, w_in, w_out)

    return jax.shard_map(local_step, mesh=mesh, in_specs=(row_spec, row_spec, expert_spec, expert_spec),
                         out_specs=row_spec, check_vma=False)
```

```python
import functools

import jax
import jax.numpy as jnp
from jax import lax
from jax.experimental import pallas as pl
from jax.experimental.pallas import tpu as pltpu
from jax.sharding import PartitionSpec as P

MESH = pl.DeviceIdType.MESH
PARTS = 4
W2_RING = 4
UNROLL = 2
SLOTS = 8
Z_COLS = ((0, 1024), (1024, 512), (1536, 512))
X_CHUNKS = tuple((i * 256, 256) for i in range(6)) + ((1536, 512),)
PROMPT = 12
DEFER = 8
AHEAD = 2


def moe_kernel(cfg, x_hbm, logits_hbm, w1_hbm, w2_hbm, out_ref,
               logits_ref, x_all, slot_tok, pos_all, ahead, mask_out, masks, rows_in, hid, z_out, z_in, mix, gates, pick_in, pick_out,
               w1_buf, w2_buf,
               w1_sem, w2_sem, own_sem, x_send, x_recv, f_recv, m_send, m_recv, ahead_recv, z_send, z_recv):
    tok, d_model, d_ff, experts, exp_dev, cap = cfg
    me = lax.axis_index("ep")
    core = me % 2
    partner = me + 1 - 2 * core
    xn = (me + 2) % 4
    diag = 3 - me
    peers = (xn, diag, partner)
    bf16, f32 = jnp.bfloat16, jnp.float32
    part = d_model // PARTS
    pairs = exp_dev // 2
    row16 = 2 * SLOTS

    def remote(src, dst, send, recv, dev):
        return pltpu.make_async_remote_copy(src_ref=src, dst_ref=dst, send_sem=send, recv_sem=recv,
                                            device_id={"ep": dev}, device_id_type=MESH)

    barrier = pltpu.get_barrier_semaphore()
    for peer in peers:
        pl.semaphore_signal(barrier, inc=1, device_id={"ep": peer}, device_id_type=MESH)
    own = pltpu.make_async_copy(x_hbm, x_all.at[pl.ds(pl.multiple_of(me * tok, tok), tok)], own_sem.at[0])
    own.start()
    get_logits = pltpu.make_async_copy(logits_hbm, logits_ref, own_sem.at[1])
    get_logits.start()

    def w1_copy(c, q, to=None):
        to = q if to is None else to
        rows = pl.ds(pl.multiple_of(c * part, part), part)
        return pltpu.make_async_copy(w1_hbm.at[pl.ds(2 * q, 2), rows], w1_buf.at[to], w1_sem.at[to])

    def w2_copy(e):
        return pltpu.make_async_copy(w2_hbm.at[e], w2_buf.at[e % W2_RING], w2_sem.at[e % W2_RING])

    def w1_start(q, carry):
        w1_copy(0, q).start()
        return carry

    lax.fori_loop(0, 2, w1_start, 0)

    def x_block(dev):
        return pl.ds(pl.multiple_of(dev * tok, tok), tok)

    def x_far(k):
        cols = pl.ds(*X_CHUNKS[k])
        mine = x_all.at[x_block(me), cols]
        return remote(mine, mine, x_send, x_recv.at[k], xn)

    def x_fwd(k):
        here = x_all.at[x_block(xn), pl.ds(*X_CHUNKS[k])]
        return remote(here, here, x_send, f_recv.at[X_CHUNKS[k][0] // part], partner)

    block = x_all.at[x_block(me)]
    x_near = remote(block, block, x_send, own_sem.at[2], partner)
    pl.semaphore_wait(barrier, 3)
    own.wait()
    x_far(0).start()
    x_near.start()

    get_logits.wait()
    logits = logits_ref[...]
    top1 = jnp.max(logits, axis=1, keepdims=True)
    is1 = logits == top1
    rest = jnp.where(is1, -jnp.inf, logits)
    top2 = jnp.max(rest, axis=1, keepdims=True)
    is2 = rest == top2
    chosen = jnp.where(is1 | is2, 1.0, 0.0)
    row_id = lax.broadcasted_iota(jnp.int32, (tok, tok), 0)
    col_id = lax.broadcasted_iota(jnp.int32, (tok, tok), 1)
    upper = jnp.where(row_id < col_id, 1.0, 0.0).astype(bf16)
    chosen_t = chosen.T
    pos = jnp.dot(chosen_t.astype(bf16), upper, preferred_element_type=f32)
    pos = jnp.where(chosen_t > 0.5, pos, -1.0)
    slot_id = lax.broadcasted_iota(jnp.int32, (experts, SLOTS, tok), 1).astype(f32)
    hot = jnp.where(pos[:, None, :] == slot_id, 1.0, 0.0).reshape(experts * SLOTS, tok).astype(bf16)
    tok_id = (lax.broadcasted_iota(jnp.int32, (8, tok), 1) + 1).astype(f32).astype(bf16)
    slot_tok[...] = lax.dot_general(tok_id, hot, (((1,), (1,)), ((), ())), preferred_element_type=f32).astype(bf16)
    counts = jnp.sum(chosen, axis=0, keepdims=True)
    counts = jnp.broadcast_to(jnp.concatenate([counts] * (tok // experts), axis=1), (8, tok))
    top_row = lax.broadcasted_iota(jnp.int32, (8, tok), 0) == 0
    mine_slots = exp_dev * SLOTS
    for i, dev in enumerate(peers + (me,)):
        lanes = pl.ds(pl.multiple_of(dev * mine_slots, mine_slots), mine_slots)
        mask_out[i] = jnp.where(top_row, slot_tok[:, lanes].astype(f32), counts).astype(bf16)
    masks[me] = mask_out[3]

    def mask_copy(i):
        return remote(mask_out.at[i], masks.at[me], m_send.at[0], m_recv.at[i], peers[i])

    for i in range(3):
        mask_copy(i).start()
    for k in range(1, len(X_CHUNKS) - 1):
        x_far(k).start()

    last = len(X_CHUNKS) - 1
    last_cols = pl.ds(*X_CHUNKS[last])

    def ahead_copy(i, dev):
        dst = rows_in.at[pl.ds(0, AHEAD), pl.ds(pl.multiple_of(dev * row16, row16), row16), last_cols]
        return remote(ahead.at[i], dst, m_send.at[1], ahead_recv.at[i], peers[i])

    pos_all[...] = pos
    for i in range(2):
        few = pos_all[pl.ds(pl.multiple_of(peers[i] * exp_dev, exp_dev), 8), :][:2 * AHEAD]
        few_id = lax.broadcasted_iota(jnp.int32, (2 * AHEAD, SLOTS, tok), 1).astype(f32)
        few = jnp.where(few[:, None, :] == few_id, 1.0, 0.0).reshape(2 * AHEAD * SLOTS, tok).astype(bf16)
        rows = jnp.dot(few, x_all[x_block(me), last_cols], preferred_element_type=f32)
        ahead[i] = rows.astype(bf16).reshape(AHEAD, row16, rows.shape[1])
    for i in range(2):
        ahead_copy(i, me).start()
    x_far(last).start()
    lax.fori_loop(2, pairs, w1_start, 0)
    for e in range(W2_RING):
        w2_copy(e).start()

    lower = jnp.where(col_id < row_id, 1.0, 0.0).astype(bf16)
    before = jnp.dot(lower, chosen.astype(bf16), preferred_element_type=f32)
    total = jnp.sum(jnp.exp(logits - top1), axis=1, keepdims=True)
    gates[0] = jnp.broadcast_to(1.0 / total, (tok, 128))
    gates[1] = jnp.broadcast_to(jnp.exp(top2 - top1) / total, (tok, 128))
    mix[...] = jnp.zeros_like(mix)

    tok_row = (row_id + 1).astype(f32)

    def picks(dev):
        hot = jnp.where(tok_row == masks[dev, 0:1, :].astype(f32), 1.0, 0.0)
        pick_in[dev] = hot.T.astype(bf16)

    def gather(dev, first, width, lo=0):
        cols = slice(first, first + width)
        rows = jnp.dot(pick_in[dev], x_all[x_block(dev), cols], preferred_element_type=f32).astype(bf16)
        rows = rows.reshape(pairs, row16, width)[lo:]
        rows_in[lo:, pl.ds(pl.multiple_of(dev * row16, row16), row16), cols] = rows

    picks(me)
    for j in range(0, d_model, 512):
        gather(me, j, 512)
    remote(mask_out.at[2], masks.at[partner], m_send.at[0], m_recv.at[2], partner).wait_recv()
    picks(partner)
    x_near.wait_recv()
    for j in range(0, d_model, 512):
        gather(partner, j, 512)
    for i in range(2):
        remote(mask_out.at[i], masks.at[peers[i]], m_send.at[0], m_recv.at[i], peers[i]).wait_recv()
        picks(peers[i])

    def pass_on(k):
        x_far(k).wait_recv()
        x_fwd(k).start()

    def gather_far(k, lo=0):
        gather(xn, *X_CHUNKS[k], lo)
        x_fwd(k).wait_recv()
        gather(diag, *X_CHUNKS[k], lo)

    pass_on(0)

    offset = jnp.zeros((1, experts), f32)
    for d in range(4):
        offset = offset + jnp.where(d < me, 1.0, 0.0) * masks[d, :, :experts].astype(f32)[1:2]
    position = before + offset
    lane = lax.broadcasted_iota(jnp.int32, (tok, experts), 1)
    dev_id, exp_id = lane // exp_dev, lane % exp_dev
    base = (((exp_id // 4) * 4 + dev_id) * 4 + exp_id % 4) * SLOTS
    base = base.astype(f32) + before
    slot_lane = lax.broadcasted_iota(jnp.int32, (tok, experts * SLOTS), 1).astype(f32)
    for i, hot in enumerate((is1, is2)):
        pos = jnp.sum(jnp.where(hot, position, 0.0), axis=1, keepdims=True)
        slot = jnp.sum(jnp.where(hot, base, 0.0), axis=1, keepdims=True)
        slot = jnp.where(pos < cap, slot, -1.0)
        pick_out[i * tok:(i + 1) * tok, :] = jnp.where(slot_lane == slot, 1.0, 0.0).astype(bf16)

    def weave(a, b):
        blocks = []
        for d in range(4):
            blocks += [a[d * row16:d * row16 + SLOTS], b[d * row16 + SLOTS:(d + 1) * row16]]
        return jnp.concatenate(blocks, axis=0)

    def first_part(c, q, at=None):
        at = q if at is None else at
        rows = rows_in[q, :, c * part:(c + 1) * part]
        both = jnp.concatenate([w1_buf[at, 0], w1_buf[at, 1]], axis=1)
        h = jnp.dot(rows, both, preferred_element_type=f32)
        return weave(h[:, :d_ff], h[:, d_ff:])

    early = AHEAD
    for c in range(PARTS):
        if c == PARTS - 1:
            for i in range(2):
                ahead_copy(i, peers[i]).wait_recv()
            break
        if c == 0:
            pass_on(1)
        there = x_all.at[x_block(diag), pl.ds(c * part, part)]
        remote(there, there, x_send, f_recv.at[c], partner).wait_recv()
        for dev in (xn, diag):
            gather(dev, c * part, part)
        def first_product(g, carry):
            for i in range(UNROLL):
                w1_copy(c, g * UNROLL + i).wait()
            for i in range(UNROLL):
                q = g * UNROLL + i
                h = first_part(c, q)
                hid[q] = h if c == 0 else hid[q] + h
            for i in range(UNROLL):
                refill(c, g * UNROLL + i)
            return carry

        def refill(c, q):
            if c < PARTS - 3:
                w1_copy(c + 1, q).start()
            elif c == PARTS - 3:
                mid = (q >= early) & (q < 2 * early)

                @pl.when(q < PROMPT)
                def _():
                    w1_copy(jnp.where(mid, PARTS - 1, PARTS - 2), jnp.where(mid, q - early, q), q).start()
            else:
                w1_copy(PARTS - 2, q + early, q).start()

        steps = (pairs if c < PARTS - 2 else early) // UNROLL
        if c == PARTS - 2:
            lax.fori_loop(0, steps, first_product, 0)
            continue
        lax.fori_loop(0, steps // 2, first_product, 0)
        pass_on(2 * c + 2)
        lax.fori_loop(steps // 2, steps * 7 // 8, first_product, 0)
        pass_on(2 * c + 3)
        lax.fori_loop(steps * 7 // 8, steps, first_product, 0)

    units = pairs // 2
    whole = pl.ds(0, d_model)

    def z_rows(dev, q):
        return pl.ds(pl.multiple_of((((q // 2) * 4 + dev) * 2 + q % 2) * row16, row16), row16)

    def z_copy(i, q, c):
        cols = pl.ds(*Z_COLS[c])
        src = z_out.at[q, pl.ds(pl.multiple_of(peers[i] * row16, row16), row16), cols]
        return remote(src, z_in.at[z_rows(me, q), cols], z_send, z_recv.at[z_id(q // 2, c)], peers[i])

    def z_id(u, c):
        return u + jnp.where(u == units - 1, c, 0)

    def unit_wait(u, cols, c):
        here = z_in.at[pl.ds(0, 6 * row16), cols]
        remote(here, here, z_send, z_recv.at[z_id(u, c)], xn).wait_recv()

    def send(q, c):
        for i in range(3):
            z_copy(i, q, c).start()

    def combine(first, depth, lo, hi):
        rows = pl.ds(pl.multiple_of(first, 128), depth)
        block = 512
        gate1 = jnp.concatenate([gates[0]] * (block // 128), axis=1)
        gate2 = jnp.concatenate([gates[1]] * (block // 128), axis=1)
        for j in range(lo, hi, block):
            cols = slice(j, j + block)
            back = jnp.dot(pick_out[:, rows], z_in[rows, cols], preferred_element_type=f32)
            mix[:, cols] += gate1 * back[:tok] + gate2 * back[tok:]

    unit = 4 * 2 * row16

    def finish(q, h):
        hidden = jax.nn.gelu(h, approximate=True).astype(bf16)
        for i in range(2):
            w2_copy(2 * q + i).wait()
        mine = pl.ds(pl.multiple_of(me * row16, row16), row16)
        for c, (lo, size) in enumerate(Z_COLS):
            cols = slice(lo, lo + size)
            a = jnp.dot(hidden, w2_buf[(2 * q) % W2_RING, :, cols], preferred_element_type=f32)
            b = jnp.dot(hidden, w2_buf[(2 * q + 1) % W2_RING, :, cols], preferred_element_type=f32)
            z_out[q, :, cols] = weave(a, b).astype(bf16)
            z_in[z_rows(me, q), cols] = z_out[q, mine, cols]
            send(q, c)
        for i in range(2):
            @pl.when(2 * q + i + W2_RING < exp_dev)
            def _():
                w2_copy(2 * q + i + W2_RING).start()

    def units_in(first, count):
        for i in range(count):
            unit_wait(first + i, whole, 0)
        combine(first * unit, count * unit, 0, d_model)

    def early_pair(q, carry):
        w1_copy(PARTS - 1, q, q + early).wait()
        h = hid[q] + first_part(PARTS - 1, q, q + early)
        w1_copy(PARTS - 1, q + early, q + early).start()
        finish(q, h)

        @pl.when(q == AHEAD - 1)
        def _():
            pass_on(last)
            gather_far(last, AHEAD)
        return carry

    def late_pair(q, carry):
        mid = q < 2 * early
        slot_a = jnp.where(mid, q - early, q)
        slot_b = jnp.where(mid, q, q - 2 * early)
        w1_copy(PARTS - 2, q, slot_a).wait()

        @pl.when((q + DEFER >= PROMPT) & (q + DEFER < pairs))
        def _():
            w1_copy(PARTS - 2, q + DEFER, q + DEFER).start()

        h = hid[q] + first_part(PARTS - 2, q, slot_a)
        w1_copy(PARTS - 1, q, slot_b).wait()
        h = h + first_part(PARTS - 1, q, slot_b)

        @pl.when(mid)
        def _():
            w1_copy(PARTS - 1, q + early, slot_a).start()
            w1_copy(PARTS - 1, q + 2 * early, slot_b).start()

        @pl.when((q >= 2 * early) & (q + 2 * early < pairs))
        def _():
            w1_copy(PARTS - 1, q + 2 * early, slot_a).start()

        finish(q, h)

        @pl.when((q == 8) | (q == 13))
        def _():
            units_in((q - 8) // 5 * 2, 2)
        return carry

    lax.fori_loop(0, early, early_pair, 0)
    lax.fori_loop(early, pairs, late_pair, 0)

    def later(u, carry):
        units_in(u, 1)
        return carry

    lax.fori_loop(units // 2, units - 1, later, 0)
    three = x_all.at[pl.ds(0, 3 * tok)]
    remote(three, three, x_send, own_sem.at[2], xn).wait_send()
    remote(mask_out.at[pl.ds(0, 3)], mask_out.at[pl.ds(0, 3)], m_send.at[0], own_sem.at[2], xn).wait_send()
    remote(ahead, ahead, m_send.at[1], own_sem.at[2], xn).wait_send()

    for c, (lo, size) in enumerate(Z_COLS):
        unit_wait(units - 1, pl.ds(lo, size), c)
        combine((units - 1) * unit, unit, lo, lo + size)
        cols = pl.ds(lo, size)
        out_ref[:, cols] = (x_all[x_block(me), cols].astype(f32) + mix[:, cols]).astype(bf16)
    remote(three, three, z_send, own_sem.at[2], xn).wait_send()


def solution(mesh):
    group = mesh.shape["ep"]
    row_spec = P(("dp", "ep"), None)
    expert_spec = P("ep", None, None)

    def local_step(x_rows, logits, w_in, w_out):
        tok, d_model = x_rows.shape
        experts = logits.shape[1]
        exp_dev, _, d_ff = w_in.shape
        cap = 2 * tok * group // experts
        cfg = (tok, d_model, d_ff, experts, exp_dev, cap)
        bf16 = jnp.bfloat16
        hbm = pl.BlockSpec(memory_space=pl.ANY)
        f32 = jnp.float32
        dma = pltpu.SemaphoreType.DMA
        return pl.pallas_call(
            functools.partial(moe_kernel, cfg),
            name="moe",
            out_shape=pltpu.VMEM((tok, d_model), bf16),
            in_specs=[hbm, hbm, hbm, hbm],
            out_specs=pl.BlockSpec(memory_space=pltpu.VMEM),
            scratch_shapes=[
                pltpu.VMEM((tok, experts), f32),
                pltpu.VMEM((group * tok, d_model), bf16),
                pltpu.VMEM((8, experts * SLOTS), bf16),
                pltpu.VMEM((experts, tok), f32),
                pltpu.VMEM((2, AHEAD, 2 * SLOTS, X_CHUNKS[-1][1]), bf16),
                pltpu.VMEM((group, 8, tok), bf16),
                pltpu.VMEM((group, 8, tok), bf16),
                pltpu.VMEM((exp_dev // 2, group * 2 * SLOTS, d_model), bf16),
                pltpu.VMEM((exp_dev // 2, group * 2 * SLOTS, d_ff), f32),
                pltpu.VMEM((exp_dev // 2, group * 2 * SLOTS, d_model), bf16),
                pltpu.VMEM((experts * SLOTS, d_model), bf16),
                pltpu.VMEM((tok, d_model), f32),
                pltpu.VMEM((2, tok, 128), f32),
                pltpu.VMEM((group, exp_dev * SLOTS, tok), bf16),
                pltpu.VMEM((2 * tok, experts * SLOTS), bf16),
                pltpu.VMEM((exp_dev // 2, 2, d_model // PARTS, d_ff), bf16),
                pltpu.VMEM((W2_RING, d_ff, d_model), bf16),
                dma((exp_dev // 2,)), dma((W2_RING,)), dma((3,)),
                dma, dma((len(X_CHUNKS),)), dma((PARTS,)),
                dma((2,)), dma((3,)), dma((2,)),
                dma, dma((exp_dev // 4 + len(Z_COLS) - 1,)),
            ],
            compiler_params=pltpu.CompilerParams(
                collective_id=0, has_side_effects=True, vmem_limit_bytes=64_500_000),
        )(x_rows, logits, w_in, w_out)

    return jax.shard_map(local_step, mesh=mesh, in_specs=(row_spec, row_spec, expert_spec, expert_spec),
                         out_specs=row_spec, check_vma=False)
```

```python
import functools

import jax
import jax.numpy as jnp
from jax import lax
from jax.experimental import pallas as pl
from jax.experimental.pallas import tpu as pltpu
from jax.sharding import PartitionSpec as P

MESH = pl.DeviceIdType.MESH
PARTS = 4
W2_RING = 4
UNROLL = 2
SLOTS = 8
Z_COLS = ((0, 1024), (1024, 512), (1536, 512))
X_CHUNKS = tuple((i * 256, 256) for i in range(6)) + ((1536, 512),)
PROMPT = 12
DEFER = 8
AHEAD = 2


def moe_kernel(cfg, x_hbm, logits_hbm, w1_hbm, w2_hbm, out_ref,
               logits_ref, x_all, slot_tok, pos_all, ahead, mask_out, masks, rows_in, hid, z_out, z_in, mix, gates, pick_in, pick_out,
               w1_buf, w2_buf,
               w1_sem, w2_sem, own_sem, x_send, x_recv, f_recv, m_send, m_recv, ahead_recv, z_send, z_recv):
    tok, d_model, d_ff, experts, exp_dev, cap = cfg
    me = lax.axis_index("ep")
    core = me % 2
    partner = me + 1 - 2 * core
    xn = (me + 2) % 4
    diag = 3 - me
    peers = (xn, diag, partner)
    bf16, f32 = jnp.bfloat16, jnp.float32
    part = d_model // PARTS
    pairs = exp_dev // 2
    row16 = 2 * SLOTS

    def remote(src, dst, send, recv, dev):
        return pltpu.make_async_remote_copy(src_ref=src, dst_ref=dst, send_sem=send, recv_sem=recv,
                                            device_id={"ep": dev}, device_id_type=MESH)

    barrier = pltpu.get_barrier_semaphore()
    for peer in peers:
        pl.semaphore_signal(barrier, inc=1, device_id={"ep": peer}, device_id_type=MESH)
    own = pltpu.make_async_copy(x_hbm, x_all.at[pl.ds(pl.multiple_of(me * tok, tok), tok)], own_sem.at[0])
    own.start()
    get_logits = pltpu.make_async_copy(logits_hbm, logits_ref, own_sem.at[1])
    get_logits.start()

    def w1_copy(c, q, to=None):
        to = q if to is None else to
        rows = pl.ds(pl.multiple_of(c * part, part), part)
        return pltpu.make_async_copy(w1_hbm.at[pl.ds(2 * q, 2), rows], w1_buf.at[to], w1_sem.at[to])

    def w2_copy(e):
        return pltpu.make_async_copy(w2_hbm.at[e], w2_buf.at[e % W2_RING], w2_sem.at[e % W2_RING])

    def w1_start(q, carry):
        w1_copy(0, q).start()
        return carry

    lax.fori_loop(0, 2, w1_start, 0)

    def x_block(dev):
        return pl.ds(pl.multiple_of(dev * tok, tok), tok)

    def x_far(k):
        cols = pl.ds(*X_CHUNKS[k])
        mine = x_all.at[x_block(me), cols]
        return remote(mine, mine, x_send, x_recv.at[k], xn)

    def x_fwd(k):
        here = x_all.at[x_block(xn), pl.ds(*X_CHUNKS[k])]
        return remote(here, here, x_send, f_recv.at[X_CHUNKS[k][0] // part], partner)

    block = x_all.at[x_block(me)]
    x_near = remote(block, block, x_send, own_sem.at[2], partner)
    pl.semaphore_wait(barrier, 3)
    own.wait()
    x_far(0).start()
    x_near.start()

    get_logits.wait()
    logits = logits_ref[...]
    top1 = jnp.max(logits, axis=1, keepdims=True)
    is1 = logits == top1
    rest = jnp.where(is1, -jnp.inf, logits)
    top2 = jnp.max(rest, axis=1, keepdims=True)
    is2 = rest == top2
    chosen = jnp.where(is1 | is2, 1.0, 0.0)
    row_id = lax.broadcasted_iota(jnp.int32, (tok, tok), 0)
    col_id = lax.broadcasted_iota(jnp.int32, (tok, tok), 1)
    upper = jnp.where(row_id < col_id, 1.0, 0.0).astype(bf16)
    chosen_t = chosen.T
    pos = jnp.dot(chosen_t.astype(bf16), upper, preferred_element_type=f32)
    pos = jnp.where(chosen_t > 0.5, pos, -1.0)
    slot_id = lax.broadcasted_iota(jnp.int32, (experts, SLOTS, tok), 1).astype(f32)
    hot = jnp.where(pos[:, None, :] == slot_id, 1.0, 0.0).reshape(experts * SLOTS, tok).astype(bf16)
    tok_id = (lax.broadcasted_iota(jnp.int32, (8, tok), 1) + 1).astype(f32).astype(bf16)
    slot_tok[...] = lax.dot_general(tok_id, hot, (((1,), (1,)), ((), ())), preferred_element_type=f32).astype(bf16)
    counts = jnp.sum(chosen, axis=0, keepdims=True)
    counts = jnp.broadcast_to(jnp.concatenate([counts] * (tok // experts), axis=1), (8, tok))
    top_row = lax.broadcasted_iota(jnp.int32, (8, tok), 0) == 0
    mine_slots = exp_dev * SLOTS
    for i, dev in enumerate(peers + (me,)):
        lanes = pl.ds(pl.multiple_of(dev * mine_slots, mine_slots), mine_slots)
        mask_out[i] = jnp.where(top_row, slot_tok[:, lanes].astype(f32), counts).astype(bf16)
    masks[me] = mask_out[3]

    def mask_copy(i):
        return remote(mask_out.at[i], masks.at[me], m_send.at[0], m_recv.at[i], peers[i])

    for i in range(3):
        mask_copy(i).start()
    for k in range(1, len(X_CHUNKS) - 1):
        x_far(k).start()

    last = len(X_CHUNKS) - 1
    last_cols = pl.ds(*X_CHUNKS[last])

    def ahead_copy(i, dev):
        dst = rows_in.at[pl.ds(0, AHEAD), pl.ds(pl.multiple_of(dev * row16, row16), row16), last_cols]
        return remote(ahead.at[i], dst, m_send.at[1], ahead_recv, peers[i])

    pos_all[...] = pos
    for i in range(2):
        few = pos_all[pl.ds(pl.multiple_of(peers[i] * exp_dev, exp_dev), 8), :][:2 * AHEAD]
        few_id = lax.broadcasted_iota(jnp.int32, (2 * AHEAD, SLOTS, tok), 1).astype(f32)
        few = jnp.where(few[:, None, :] == few_id, 1.0, 0.0).reshape(2 * AHEAD * SLOTS, tok).astype(bf16)
        rows = jnp.dot(few, x_all[x_block(me), last_cols], preferred_element_type=f32)
        ahead[i] = rows.astype(bf16).reshape(AHEAD, row16, rows.shape[1])
    for i in range(2):
        ahead_copy(i, me).start()
    x_far(last).start()
    lax.fori_loop(2, pairs, w1_start, 0)
    for e in range(W2_RING):
        w2_copy(e).start()

    lower = jnp.where(col_id < row_id, 1.0, 0.0).astype(bf16)
    before = jnp.dot(lower, chosen.astype(bf16), preferred_element_type=f32)
    total = jnp.sum(jnp.exp(logits - top1), axis=1, keepdims=True)
    gates[0] = jnp.broadcast_to(1.0 / total, (tok, 128))
    gates[1] = jnp.broadcast_to(jnp.exp(top2 - top1) / total, (tok, 128))
    mix[...] = jnp.zeros_like(mix)

    tok_row = (row_id + 1).astype(f32)

    def picks(dev):
        hot = jnp.where(tok_row == masks[dev, 0:1, :].astype(f32), 1.0, 0.0)
        pick_in[dev] = hot.T.astype(bf16)

    def gather(dev, first, width, lo=0):
        cols = slice(first, first + width)
        rows = jnp.dot(pick_in[dev], x_all[x_block(dev), cols], preferred_element_type=f32).astype(bf16)
        rows = rows.reshape(pairs, row16, width)[lo:]
        rows_in[lo:, pl.ds(pl.multiple_of(dev * row16, row16), row16), cols] = rows

    picks(me)
    for j in range(0, d_model, 512):
        gather(me, j, 512)
    remote(mask_out.at[2], masks.at[partner], m_send.at[0], m_recv.at[2], partner).wait_recv()
    picks(partner)
    x_near.wait_recv()
    for j in range(0, d_model, 512):
        gather(partner, j, 512)
    for i in range(2):
        remote(mask_out.at[i], masks.at[peers[i]], m_send.at[0], m_recv.at[i], peers[i]).wait_recv()
        picks(peers[i])

    def pass_on(k):
        x_far(k).wait_recv()
        x_fwd(k).start()

    def gather_far(k, lo=0):
        gather(xn, *X_CHUNKS[k], lo)
        x_fwd(k).wait_recv()
        gather(diag, *X_CHUNKS[k], lo)

    pass_on(0)

    offset = jnp.zeros((1, experts), f32)
    for d in range(4):
        offset = offset + jnp.where(d < me, 1.0, 0.0) * masks[d, :, :experts].astype(f32)[1:2]
    position = before + offset
    lane = lax.broadcasted_iota(jnp.int32, (tok, experts), 1)
    dev_id, exp_id = lane // exp_dev, lane % exp_dev
    base = (((exp_id // 4) * 4 + dev_id) * 4 + exp_id % 4) * SLOTS
    base = base.astype(f32) + before
    slot_lane = lax.broadcasted_iota(jnp.int32, (tok, experts * SLOTS), 1).astype(f32)
    for i, hot in enumerate((is1, is2)):
        pos = jnp.sum(jnp.where(hot, position, 0.0), axis=1, keepdims=True)
        slot = jnp.sum(jnp.where(hot, base, 0.0), axis=1, keepdims=True)
        slot = jnp.where(pos < cap, slot, -1.0)
        pick_out[i * tok:(i + 1) * tok, :] = jnp.where(slot_lane == slot, 1.0, 0.0).astype(bf16)

    def weave(a, b):
        blocks = []
        for d in range(4):
            blocks += [a[d * row16:d * row16 + SLOTS], b[d * row16 + SLOTS:(d + 1) * row16]]
        return jnp.concatenate(blocks, axis=0)

    def first_part(c, q, at=None):
        at = q if at is None else at
        rows = rows_in[q, :, c * part:(c + 1) * part]
        both = jnp.concatenate([w1_buf[at, 0], w1_buf[at, 1]], axis=1)
        h = jnp.dot(rows, both, preferred_element_type=f32)
        return weave(h[:, :d_ff], h[:, d_ff:])

    early = AHEAD
    for c in range(PARTS):
        if c == PARTS - 1:
            remote(ahead, ahead, m_send.at[1], ahead_recv, xn).wait_recv()
            break
        if c == 0:
            pass_on(1)
        there = x_all.at[x_block(diag), pl.ds(c * part, part)]
        remote(there, there, x_send, f_recv.at[c], partner).wait_recv()
        for dev in (xn, diag):
            gather(dev, c * part, part)
        def first_product(g, carry):
            for i in range(UNROLL):
                w1_copy(c, g * UNROLL + i).wait()
            for i in range(UNROLL):
                q = g * UNROLL + i
                h = first_part(c, q)
                hid[q] = h if c == 0 else hid[q] + h
            for i in range(UNROLL):
                refill(c, g * UNROLL + i)
            return carry

        def refill(c, q):
            if c < PARTS - 3:
                w1_copy(c + 1, q).start()
            elif c == PARTS - 3:
                mid = (q >= early) & (q < 2 * early)

                @pl.when(q < PROMPT)
                def _():
                    w1_copy(jnp.where(mid, PARTS - 1, PARTS - 2), jnp.where(mid, q - early, q), q).start()
            else:
                w1_copy(PARTS - 2, q + early, q).start()

        steps = (pairs if c < PARTS - 2 else early) // UNROLL
        if c == PARTS - 2:
            lax.fori_loop(0, steps, first_product, 0)
            continue
        lax.fori_loop(0, steps // 2, first_product, 0)
        pass_on(2 * c + 2)
        lax.fori_loop(steps // 2, steps * 7 // 8, first_product, 0)
        pass_on(2 * c + 3)
        lax.fori_loop(steps * 7 // 8, steps, first_product, 0)

    units = pairs // 2
    whole = pl.ds(0, d_model)

    def z_rows(dev, q):
        return pl.ds(pl.multiple_of((((q // 2) * 4 + dev) * 2 + q % 2) * row16, row16), row16)

    def z_copy(i, q, c):
        cols = pl.ds(*Z_COLS[c])
        src = z_out.at[q, pl.ds(pl.multiple_of(peers[i] * row16, row16), row16), cols]
        return remote(src, z_in.at[z_rows(me, q), cols], z_send, z_recv.at[z_id(q // 2, c)], peers[i])

    def z_id(u, c):
        return u + jnp.where(u == units - 1, c, 0)

    def unit_wait(u, cols, c):
        here = z_in.at[pl.ds(0, 6 * row16), cols]
        remote(here, here, z_send, z_recv.at[z_id(u, c)], xn).wait_recv()

    def send(q, c):
        for i in range(3):
            z_copy(i, q, c).start()

    def combine(first, depth, lo, hi):
        rows = pl.ds(pl.multiple_of(first, 128), depth)
        block = 512
        gate1 = jnp.concatenate([gates[0]] * (block // 128), axis=1)
        gate2 = jnp.concatenate([gates[1]] * (block // 128), axis=1)
        for j in range(lo, hi, block):
            cols = slice(j, j + block)
            back = jnp.dot(pick_out[:, rows], z_in[rows, cols], preferred_element_type=f32)
            mix[:, cols] += gate1 * back[:tok] + gate2 * back[tok:]

    unit = 4 * 2 * row16

    def finish(q, h):
        hidden = jax.nn.gelu(h, approximate=True).astype(bf16)
        for i in range(2):
            w2_copy(2 * q + i).wait()
        mine = pl.ds(pl.multiple_of(me * row16, row16), row16)
        for c, (lo, size) in enumerate(Z_COLS):
            cols = slice(lo, lo + size)
            a = jnp.dot(hidden, w2_buf[(2 * q) % W2_RING, :, cols], preferred_element_type=f32)
            b = jnp.dot(hidden, w2_buf[(2 * q + 1) % W2_RING, :, cols], preferred_element_type=f32)
            z_out[q, :, cols] = weave(a, b).astype(bf16)
            z_in[z_rows(me, q), cols] = z_out[q, mine, cols]
            send(q, c)
        for i in range(2):
            @pl.when(2 * q + i + W2_RING < exp_dev)
            def _():
                w2_copy(2 * q + i + W2_RING).start()

    def units_in(first, count):
        for i in range(count):
            unit_wait(first + i, whole, 0)
        combine(first * unit, count * unit, 0, d_model)

    def early_pair(q, carry):
        w1_copy(PARTS - 1, q, q + early).wait()
        h = hid[q] + first_part(PARTS - 1, q, q + early)
        w1_copy(PARTS - 1, q + early, q + early).start()
        finish(q, h)

        @pl.when(q == AHEAD - 1)
        def _():
            pass_on(last)
            gather_far(last, AHEAD)
        return carry

    def late_pair(q, carry):
        mid = q < 2 * early
        slot_a = jnp.where(mid, q - early, q)
        slot_b = jnp.where(mid, q, q - 2 * early)
        w1_copy(PARTS - 2, q, slot_a).wait()

        @pl.when((q + DEFER >= PROMPT) & (q + DEFER < pairs))
        def _():
            w1_copy(PARTS - 2, q + DEFER, q + DEFER).start()

        h = hid[q] + first_part(PARTS - 2, q, slot_a)
        w1_copy(PARTS - 1, q, slot_b).wait()
        h = h + first_part(PARTS - 1, q, slot_b)

        @pl.when(mid)
        def _():
            w1_copy(PARTS - 1, q + early, slot_a).start()
            w1_copy(PARTS - 1, q + 2 * early, slot_b).start()

        @pl.when((q >= 2 * early) & (q + 2 * early < pairs))
        def _():
            w1_copy(PARTS - 1, q + 2 * early, slot_a).start()

        finish(q, h)

        @pl.when((q == 8) | (q == 13))
        def _():
            units_in((q - 8) // 5 * 2, 2)
        return carry

    lax.fori_loop(0, early, early_pair, 0)
    lax.fori_loop(early, pairs, late_pair, 0)

    def later(u, carry):
        units_in(u, 1)
        return carry

    lax.fori_loop(units // 2, units - 1, later, 0)
    three = x_all.at[pl.ds(0, 3 * tok)]
    remote(three, three, x_send, own_sem.at[2], xn).wait_send()
    remote(mask_out.at[pl.ds(0, 3)], mask_out.at[pl.ds(0, 3)], m_send.at[0], own_sem.at[2], xn).wait_send()
    remote(ahead, ahead, m_send.at[1], own_sem.at[2], xn).wait_send()

    for c, (lo, size) in enumerate(Z_COLS):
        unit_wait(units - 1, pl.ds(lo, size), c)
        combine((units - 1) * unit, unit, lo, lo + size)
        cols = pl.ds(lo, size)
        out_ref[:, cols] = (x_all[x_block(me), cols].astype(f32) + mix[:, cols]).astype(bf16)
    remote(three, three, z_send, own_sem.at[2], xn).wait_send()


def solution(mesh):
    group = mesh.shape["ep"]
    row_spec = P(("dp", "ep"), None)
    expert_spec = P("ep", None, None)

    def local_step(x_rows, logits, w_in, w_out):
        tok, d_model = x_rows.shape
        experts = logits.shape[1]
        exp_dev, _, d_ff = w_in.shape
        cap = 2 * tok * group // experts
        cfg = (tok, d_model, d_ff, experts, exp_dev, cap)
        bf16 = jnp.bfloat16
        hbm = pl.BlockSpec(memory_space=pl.ANY)
        f32 = jnp.float32
        dma = pltpu.SemaphoreType.DMA
        return pl.pallas_call(
            functools.partial(moe_kernel, cfg),
            name="moe",
            out_shape=pltpu.VMEM((tok, d_model), bf16),
            in_specs=[hbm, hbm, hbm, hbm],
            out_specs=pl.BlockSpec(memory_space=pltpu.VMEM),
            scratch_shapes=[
                pltpu.VMEM((tok, experts), f32),
                pltpu.VMEM((group * tok, d_model), bf16),
                pltpu.VMEM((8, experts * SLOTS), bf16),
                pltpu.VMEM((experts, tok), f32),
                pltpu.VMEM((2, AHEAD, 2 * SLOTS, X_CHUNKS[-1][1]), bf16),
                pltpu.VMEM((group, 8, tok), bf16),
                pltpu.VMEM((group, 8, tok), bf16),
                pltpu.VMEM((exp_dev // 2, group * 2 * SLOTS, d_model), bf16),
                pltpu.VMEM((exp_dev // 2, group * 2 * SLOTS, d_ff), f32),
                pltpu.VMEM((exp_dev // 2, group * 2 * SLOTS, d_model), bf16),
                pltpu.VMEM((experts * SLOTS, d_model), bf16),
                pltpu.VMEM((tok, d_model), f32),
                pltpu.VMEM((2, tok, 128), f32),
                pltpu.VMEM((group, exp_dev * SLOTS, tok), bf16),
                pltpu.VMEM((2 * tok, experts * SLOTS), bf16),
                pltpu.VMEM((exp_dev // 2, 2, d_model // PARTS, d_ff), bf16),
                pltpu.VMEM((W2_RING, d_ff, d_model), bf16),
                dma((exp_dev // 2,)), dma((W2_RING,)), dma((3,)),
                dma, dma((len(X_CHUNKS),)), dma((PARTS,)),
                dma((2,)), dma((3,)), dma,
                dma, dma((exp_dev // 4 + len(Z_COLS) - 1,)),
            ],
            compiler_params=pltpu.CompilerParams(
                collective_id=0, has_side_effects=True, vmem_limit_bytes=64_500_000),
        )(x_rows, logits, w_in, w_out)

    return jax.shard_map(local_step, mesh=mesh, in_specs=(row_spec, row_spec, expert_spec, expert_spec),
                         out_specs=row_spec, check_vma=False)
```
